32 devices in a mesh: dp: 1 (over z), col: 4 (over y), row: 8 (over x, core).
Axes of the slice: x: 4, y: 4, z: 1, core: 2. Of those that a mesh axis runs over, the one named last changes fastest.
The devices are a block of a 4x4x8 slice.
Arguments:
- latent: bfloat16 [2, 32, 192, 1280], P('dp', 'row', 'col')
- t_emb: bfloat16 [2, 1280], P('dp')
- res_norm: bfloat16 [2, 2, 2, 1280], replicated
- res_conv: bfloat16 [2, 2, 3, 3, 1280, 1280], replicated
- res_temb: bfloat16 [2, 1280, 1280], replicated
- attn_norm: bfloat16 [2, 1280], replicated
- attn_proj: bfloat16 [4, 20, 1280, 64], replicated
Outputs:
- output: bfloat16 [2, 32, 192, 1280], P('dp', 'row', 'col')
All inputs are finite; a program needn't handle non-finite values.
Results may differ from the reference program's by a relative error of at most 0.0117124.
Values are sent between devices in bfloat16 or wider.
A program may use at most 768 MiB of HBM per device.

```python
import jax
import jax.numpy as jnp
from jax import lax

BATCH = 2
HEIGHT = 32
WIDTH = 192
CHANNELS = 1280
HEADS = 20
TEMB_DIM = 1280
GROUPS = 32
Q_BLOCK = 192
EPS = 1e-5
HEAD_DIM = CHANNELS // HEADS


def setup_inputs(seed: int = 0, part: int = 0) -> dict:
    part_keys = jax.random.split(jax.random.fold_in(jax.random.key(seed), part), 3)
    shared_keys = jax.random.split(jax.random.key(seed + 1), 5)
    base_noise = jax.random.normal(part_keys[0], (BATCH, HEIGHT, WIDTH, CHANNELS), jnp.float32)
    slopes = 1.5 * jax.random.normal(part_keys[1], (2, BATCH, 1, 1, CHANNELS), jnp.float32)
    ramp_rows = jnp.linspace(-1.0, 1.0, HEIGHT)[None, :, None, None]
    ramp_cols = jnp.linspace(-1.0, 1.0, WIDTH)[None, None, :, None]
    latent = base_noise + slopes[0] * ramp_rows + slopes[1] * ramp_cols
    t_emb = jax.random.normal(part_keys[2], (BATCH, TEMB_DIM), jnp.float32)
    norm_draw = jax.random.normal(shared_keys[0], (2, 2, 2, CHANNELS), jnp.float32)
    res_norm = jnp.stack([1.0 + 0.3 * norm_draw[:, :, 0], 0.5 * norm_draw[:, :, 1]], axis=2)
    res_conv = jax.random.normal(shared_keys[1], (2, 2, 3, 3, CHANNELS, CHANNELS), jnp.float32) * (9 * CHANNELS) ** -0.5
    res_temb = jax.random.normal(shared_keys[2], (2, TEMB_DIM, CHANNELS), jnp.float32) * TEMB_DIM ** -0.5
    attn_draw = jax.random.normal(shared_keys[3], (2, CHANNELS), jnp.float32)
    attn_norm = jnp.stack([1.0 + 0.3 * attn_draw[0], 0.5 * attn_draw[1]])
    proj_gain = jnp.array([1.5, 1.5, 1.0, 1.5], jnp.float32)[:, None, None, None]
    attn_proj = jax.random.normal(shared_keys[4], (4, HEADS, CHANNELS, HEAD_DIM), jnp.float32) * proj_gain * CHANNELS ** -0.5
    return {
        'latent': latent.astype(jnp.bfloat16),
        't_emb': t_emb.astype(jnp.bfloat16),
        'res_norm': res_norm.astype(jnp.bfloat16),
        'res_conv': res_conv.astype(jnp.bfloat16),
        'res_temb': res_temb.astype(jnp.bfloat16),
        'attn_norm': attn_norm.astype(jnp.bfloat16),
        'attn_proj': attn_proj.astype(jnp.bfloat16),
    }


def group_norm(values, gn_scale, gn_shift):
    group_ch = CHANNELS // GROUPS
    grouped = values.astype(jnp.float32).reshape(BATCH, HEIGHT, WIDTH, GROUPS, group_ch)
    elem_count = HEIGHT * WIDTH * group_ch
    mean_val = jnp.sum(grouped, axis=(1, 2, 4)) / elem_count
    mean_sq = jnp.sum(grouped * grouped, axis=(1, 2, 4)) / elem_count
    inv_std = lax.rsqrt(mean_sq - mean_val * mean_val + EPS)
    normed = (grouped - mean_val[:, None, None, :, None]) * inv_std[:, None, None, :, None]
    return normed.reshape(values.shape) * gn_scale.astype(jnp.float32) + gn_shift.astype(jnp.float32)


def conv3x3(acts_in, kernel):
    return lax.conv_general_dilated(acts_in.astype(jnp.float32), kernel.astype(jnp.float32), (1, 1), ((1, 1), (1, 1)), dimension_numbers=('NHWC', 'HWIO', 'NHWC'))


def res_block(latent, t_emb, norm_par, kernels, w_temb):
    t_act = jax.nn.silu(t_emb.astype(jnp.float32)).astype(jnp.bfloat16)
    t_proj = jnp.dot(t_act, w_temb, preferred_element_type=jnp.float32)
    first_act = jax.nn.silu(group_norm(latent, norm_par[0, 0], norm_par[0, 1])).astype(jnp.bfloat16)
    hidden = (conv3x3(first_act, kernels[0]) + t_proj[:, None, None, :]).astype(jnp.bfloat16)
    second_act = jax.nn.silu(group_norm(hidden, norm_par[1, 0], norm_par[1, 1])).astype(jnp.bfloat16)
    return (latent.astype(jnp.float32) + conv3x3(second_act, kernels[1])).astype(jnp.bfloat16)


def attn_block(latent, norm_par, proj_w):
    n_tok = HEIGHT * WIDTH
    normed = group_norm(latent, norm_par[0], norm_par[1]).astype(jnp.bfloat16).reshape(BATCH, n_tok, CHANNELS)
    qkv_all = jnp.einsum('bnc,khcd->kbnhd', normed.astype(jnp.float32), proj_w[:3].astype(jnp.float32)).astype(jnp.bfloat16)
    q_blocks = qkv_all[0].reshape(BATCH, n_tok // Q_BLOCK, Q_BLOCK, HEADS, HEAD_DIM)
    k_all = qkv_all[1].astype(jnp.float32)
    v_all = qkv_all[2].astype(jnp.float32)

    def one_image(image_args):
        q_img, k_img, v_img = image_args

        def one_block(q_blk):
            logits = jnp.einsum('qhd,khd->hqk', q_blk.astype(jnp.float32), k_img) * HEAD_DIM ** -0.5
            att_weights = jax.nn.softmax(logits, axis=-1)
            return jnp.einsum('hqk,khd->qhd', att_weights, v_img)

        return lax.map(one_block, q_img)

    attn_out = lax.map(one_image, (q_blocks, k_all, v_all)).reshape(BATCH, n_tok, HEADS, HEAD_DIM)
    out_proj = jnp.einsum('bnhd,hcd->bnc', attn_out.astype(jnp.bfloat16).astype(jnp.float32), proj_w[3].astype(jnp.float32))
    return (latent.astype(jnp.float32) + out_proj.reshape(latent.shape)).astype(jnp.bfloat16)


def reference(latent, t_emb, res_norm, res_conv, res_temb, attn_norm, attn_proj):
    hidden = res_block(latent, t_emb, res_norm[0], res_conv[0], res_temb[0])
    hidden = attn_block(hidden, attn_norm, attn_proj)
    return res_block(hidden, t_emb, res_norm[1], res_conv[1], res_temb[1])
```

```python
import functools

import jax
import jax.numpy as jnp
from jax import lax
from jax.experimental import pallas as pl
from jax.experimental.pallas import tpu as pltpu
from jax.sharding import PartitionSpec as P

GROUPS = 32
EPS = 1e-5
LANES = 128
MESH = pl.DeviceIdType.MESH
HIGH = lax.Precision.HIGHEST
F32 = jnp.float32
BF16 = jnp.bfloat16
VMEM_LIMIT = 60 * 1024 * 1024
VSPEC = pl.BlockSpec(memory_space=pltpu.VMEM)
ASPEC = pl.BlockSpec(memory_space=pl.ANY)


def group_mask(n_chan, chan_axis):
    width = n_chan // GROUPS
    shape = (n_chan, LANES) if chan_axis == 0 else (LANES, n_chan)
    chan = lax.broadcasted_iota(jnp.int32, shape, chan_axis)
    first = lax.broadcasted_iota(jnp.int32, shape, 1 - chan_axis) * width
    return jnp.where((chan >= first) & (chan < first + width), 1.0, 0.0).astype(F32)


def channel_stats(tot, count):
    vals = tot / count
    mean = vals[0:2]
    inv = lax.rsqrt(vals[2:4] - mean * mean + EPS)
    return jnp.concatenate([mean, inv, jnp.zeros((4, LANES), F32)], axis=0)


def expand(stats, n_chan):
    return jnp.dot(stats, group_mask(n_chan, 1), precision=HIGH, preferred_element_type=F32)


def silu(u):
    half = 0.5 * u
    return half * jnp.tanh(half) + half


def finish(acc, out_ref, edge_ref, part_ref, csum):
    n_img, n_rows, n_cols, n_chan = out_ref.shape
    per_img = n_rows * n_cols
    csum[...] = jnp.zeros_like(csum)
    for ch in range(0, n_chan, 256):
        sl = slice(ch, ch + 256)
        for b in range(n_img):
            val = acc[b * per_img:(b + 1) * per_img, sl].astype(BF16)
            out_ref[b, :, :, sl] = val.reshape(n_rows, n_cols, 256)
            val = val.astype(F32)
            csum[b:b + 1, sl] = jnp.sum(val, axis=0, keepdims=True)
            csum[2 + b:3 + b, sl] = jnp.sum(val * val, axis=0, keepdims=True)
    for side, col in ((0, 0), (1, n_cols - 1)):
        for i in range(n_rows):
            rows = [acc[b * per_img + i * n_cols + col:b * per_img + i * n_cols + col + 1, :] for b in range(n_img)]
            edge_ref[side, i] = jnp.concatenate(rows, axis=0).astype(BF16)
    part_ref[...] = jnp.dot(csum[...], group_mask(n_chan, 0), precision=HIGH, preferred_element_type=F32)


def prep_kernel(x_ref, edge_ref, part_ref, acc, dump, csum):
    n_img, n_rows, n_cols, n_chan = x_ref.shape
    acc[...] = x_ref[...].reshape(acc.shape).astype(F32)
    finish(acc, dump, edge_ref, part_ref, csum)


def finish_shapes(shape):
    n_img, n_rows, n_cols, n_chan = shape
    return [jax.ShapeDtypeStruct((2, n_rows, n_img, n_chan), BF16), jax.ShapeDtypeStruct((8, LANES), F32)]


def prep(x):
    n_tok = x.shape[0] * x.shape[1] * x.shape[2]
    return pl.pallas_call(
        prep_kernel,
        out_shape=finish_shapes(x.shape),
        in_specs=[VSPEC],
        out_specs=[VSPEC, VSPEC],
        scratch_shapes=[pltpu.VMEM((n_tok, x.shape[3]), F32), pltpu.VMEM(x.shape, BF16), pltpu.VMEM((8, x.shape[3]), F32)],
        compiler_params=pltpu.CompilerParams(vmem_limit_bytes=VMEM_LIMIT),
        name="prep",
    )(x)


def exchange_kernel(n_row, n_col, halo, *refs):
    if halo:
        part_ref, x_ref, edge_ref, tot_ref, top_ref, bot_ref, side_ref, rbuf, cbuf, rsum, send, recv = refs
    else:
        part_ref, tot_ref, rbuf, cbuf, rsum, send, recv = refs
    r, c = lax.axis_index('row'), lax.axis_index('col')
    up, down = lax.rem(r + n_row - 1, n_row), lax.rem(r + 1, n_row)
    left, right = lax.rem(c + n_col - 1, n_col), lax.rem(c + 1, n_col)
    row_peers = [{'row': lax.rem(r + k, n_row)} for k in range(1, n_row)]
    col_peers = [{'col': lax.rem(c + k, n_col)} for k in range(1, n_col)]
    diag = [{'row': a, 'col': b} for a in (up, down) for b in (left, right)] if halo else []
    peers = row_peers + col_peers + diag
    barrier = pltpu.get_barrier_semaphore()
    for peer in peers:
        pl.semaphore_signal(barrier, inc=1, device_id=peer, device_id_type=MESH)
    pl.semaphore_wait(barrier, len(peers))

    def copy(src, dst, slot, peer):
        return pltpu.make_async_remote_copy(src_ref=src, dst_ref=dst, send_sem=send.at[slot], recv_sem=recv.at[slot], device_id=peer, device_id_type=MESH)

    first = [copy(part_ref, rbuf.at[k], k, row_peers[k]) for k in range(n_row - 1)]
    for cp in first:
        cp.start()
    base = n_row - 1 + n_col - 1
    halos = []
    if halo:
        last = x_ref.shape[1] - 1
        end = side_ref.shape[1] - 1
        plan = [
            (x_ref.at[:, last], top_ref, {'row': down}),
            (x_ref.at[:, 0], bot_ref, {'row': up}),
            (edge_ref.at[0], side_ref.at[1, 1:end], {'col': left}),
            (edge_ref.at[1], side_ref.at[0, 1:end], {'col': right}),
            (edge_ref.at[0, 0], side_ref.at[1, end], {'row': up, 'col': left}),
            (edge_ref.at[0, last], side_ref.at[1, 0], {'row': down, 'col': left}),
            (edge_ref.at[1, 0], side_ref.at[0, end], {'row': up, 'col': right}),
            (edge_ref.at[1, last], side_ref.at[0, 0], {'row': down, 'col': right}),
        ]
        halos = [copy(src, dst, base + i, peer) for i, (src, dst, peer) in enumerate(plan)]
        for cp in halos:
            cp.start()
    total = part_ref[...]
    for k, cp in enumerate(first):
        cp.wait_recv()
        total = total + rbuf[k]
    rsum[...] = total
    second = [copy(rsum, cbuf.at[k], n_row - 1 + k, col_peers[k]) for k in range(n_col - 1)]
    for cp in second:
        cp.start()
    for k, cp in enumerate(second):
        cp.wait_recv()
        total = total + cbuf[k]
    tot_ref[...] = total
    for cp in halos:
        cp.wait_recv()
    for cp in first + second + halos:
        cp.wait_send()


def exchange(part, n_row, n_col, x=None, edge=None):
    halo = x is not None
    out_shape = [jax.ShapeDtypeStruct((8, LANES), F32)]
    args = [part]
    in_specs = [VSPEC]
    if halo:
        n_img, n_rows, n_cols, n_chan = x.shape
        out_shape += [
            jax.ShapeDtypeStruct((n_img, n_cols, n_chan), BF16),
            jax.ShapeDtypeStruct((n_img, n_cols, n_chan), BF16),
            jax.ShapeDtypeStruct((2, n_rows + 2, n_img, n_chan), BF16),
        ]
        args += [x, edge]
        in_specs += [ASPEC, VSPEC]
    n_sem = n_row + n_col - 2 + (8 if halo else 0)
    return pl.pallas_call(
        functools.partial(exchange_kernel, n_row, n_col, halo),
        out_shape=out_shape,
        in_specs=in_specs,
        out_specs=[VSPEC] * len(out_shape),
        scratch_shapes=[
            pltpu.VMEM((n_row - 1, 8, LANES), F32),
            pltpu.VMEM((n_col - 1, 8, LANES), F32),
            pltpu.VMEM((8, LANES), F32),
            pltpu.SemaphoreType.DMA((n_sem,)),
            pltpu.SemaphoreType.DMA((n_sem,)),
        ],
        compiler_params=pltpu.CompilerParams(collective_id=1 if halo else 2, has_side_effects=True, vmem_limit_bytes=16 * 1024 * 1024),
        name="exchange",
    )(*args)


def conv_kernel(blk, idx, n_row, n_col, count, residual, x_ref, top_ref, bot_ref, side_ref, tot_ref, norm_ref, add_ref, w_hbm,
                out_ref, edge_ref, part_ref, act, hside, stat, wbuf, acc, csum, sem):
    n_img, n_rows, n_cols, n_chan = x_ref.shape
    per_img = n_rows * n_cols

    def fetch(dy):
        return pltpu.make_async_copy(w_hbm.at[blk, idx, dy], wbuf.at[dy], sem.at[dy])

    for dy in range(3):
        fetch(dy).start()
    r, c = lax.axis_index('row'), lax.axis_index('col')
    st = expand(channel_stats(tot_ref[...], count), n_chan)
    gain = norm_ref[blk, idx, 0:1, :].astype(F32)
    shift = norm_ref[blk, idx, 1:2, :].astype(F32)
    stat[0:2] = st[0:2]
    stat[2:4] = st[2:4] * gain
    stat[4:5] = shift

    for side in range(2):
        inside = (c > 0) if side == 0 else (c < n_col - 1)
        for i in range(n_rows + 2):
            ok = inside
            if i == 0:
                ok = ok & (r > 0)
            if i == n_rows + 1:
                ok = ok & (r < n_row - 1)
            z = side_ref[side, i].astype(F32)
            a = silu((z - stat[0:2]) * stat[2:4] + stat[4:5])
            hside[side, i] = jnp.where(ok, a, 0.0)

    step = 256

    def place(b, i, src, ok):
        rows = lax.broadcasted_iota(jnp.int32, (n_cols, step), 0)
        for ch in range(0, n_chan, step):
            sl = slice(ch, ch + step)
            z = src(sl).astype(F32)
            a = silu((z - stat[b:b + 1, sl]) * stat[2 + b:3 + b, sl] + stat[4:5, sl])
            if ok is not None:
                a = jnp.where(ok, a, 0.0)
            act[b, i, :, n_chan + ch:n_chan + ch + step] = a.astype(BF16)
            lo = jnp.where(rows == 0, hside[0, i, b:b + 1, sl], pltpu.roll(a, 1, 0))
            act[b, i, :, ch:ch + step] = lo.astype(BF16)
            hi = jnp.where(rows == n_cols - 1, hside[1, i, b:b + 1, sl], pltpu.roll(a, n_cols - 1, 0))
            act[b, i, :, 2 * n_chan + ch:2 * n_chan + ch + step] = hi.astype(BF16)

    for b in range(n_img):
        place(b, 0, lambda sl, b=b: top_ref[b, :, sl], r > 0)

        def middle(i, carry, b=b):
            place(b, i + 1, lambda sl: x_ref[b, i, :, sl], None)
            return carry

        lax.fori_loop(0, n_rows, middle, 0)
        place(b, n_rows + 1, lambda sl, b=b: bot_ref[b, :, sl], r < n_row - 1)

    if residual:
        acc[...] = add_ref[...].reshape(acc.shape).astype(F32)
    else:
        for b in range(n_img):
            acc[b * per_img:(b + 1) * per_img, :] = jnp.broadcast_to(add_ref[b:b + 1, :], (per_img, n_chan))

    def taps(dy, carry):
        fetch(dy).wait()
        lhs = act[:, pl.ds(dy, n_rows)].reshape(n_img * per_img, 3 * n_chan)
        for ch in range(0, n_chan, 256):
            rhs = wbuf[dy, :, :, ch:ch + 256].reshape(3 * n_chan, 256)
            acc[:, ch:ch + 256] += jnp.dot(lhs, rhs, preferred_element_type=F32)
        return carry

    lax.fori_loop(0, 3, taps, 0)
    finish(acc, out_ref, edge_ref, part_ref, csum)


def conv(blk, idx, x, halos, norm, add, weights, n_row, n_col, residual):
    tot, top, bot, side = halos
    n_img, n_rows, n_cols, n_chan = x.shape
    count = float(n_rows * n_cols * n_row * n_col * (n_chan // GROUPS))
    n_tok = n_img * n_rows * n_cols
    return pl.pallas_call(
        functools.partial(conv_kernel, blk, idx, n_row, n_col, count, residual),
        out_shape=[jax.ShapeDtypeStruct(x.shape, BF16)] + finish_shapes(x.shape),
        in_specs=[VSPEC] * 7 + [ASPEC],
        out_specs=[VSPEC] * 3,
        scratch_shapes=[
            pltpu.VMEM((n_img, n_rows + 2, n_cols, 3 * n_chan), BF16),
            pltpu.VMEM((2, n_rows + 2, n_img, n_chan), F32),
            pltpu.VMEM((8, n_chan), F32),
            pltpu.VMEM((3, 3, n_chan, n_chan), BF16),
            pltpu.VMEM((n_tok, n_chan), F32),
            pltpu.VMEM((8, n_chan), F32),
            pltpu.SemaphoreType.DMA((3,)),
        ],
        compiler_params=pltpu.CompilerParams(vmem_limit_bytes=VMEM_LIMIT),
        cost_estimate=pl.CostEstimate(flops=2 * 9 * n_tok * n_chan * n_chan, bytes_accessed=9 * 2 * n_chan * n_chan, transcendentals=n_tok * n_chan),
        name="conv",
    )(x, top, bot, side, tot, norm, add, weights)


def proj_kernel(count, per_dev, x_ref, tot_ref, norm_ref, w_ref, out_ref, g, wcat):
    n_img, n_rows, n_cols, n_chan = x_ref.shape
    per_img = n_rows * n_cols
    hd = w_ref.shape[2]

    @pl.when(pl.program_id(0) == 0)
    def _():
        st = expand(channel_stats(tot_ref[...], count), n_chan)
        gain = norm_ref[0:1, :].astype(F32)
        shift = norm_ref[1:2, :].astype(F32)
        for b in range(n_img):
            z = x_ref[b].reshape(per_img, n_chan).astype(F32)
            g[b * per_img:(b + 1) * per_img, :] = ((z - st[b:b + 1]) * (st[2 + b:3 + b] * gain) + shift).astype(BF16)
        wcat[per_dev * 3 * hd:, :] = jnp.zeros((wcat.shape[0] - per_dev * 3 * hd, n_chan), BF16)

    for i in range(per_dev):
        wcat[2 * i * hd:(2 * i + 1) * hd, :] = w_ref[1, i]
        wcat[(2 * i + 1) * hd:(2 * i + 2) * hd, :] = w_ref[2, i]
        wcat[(2 * per_dev + i) * hd:(2 * per_dev + i + 1) * hd, :] = w_ref[0, i]
    for n in range(0, wcat.shape[0], 256):
        res = lax.dot_general(g[...], wcat[n:n + 256, :], (((1,), (1,)), ((), ())), preferred_element_type=F32).astype(BF16)
        for b in range(n_img):
            out_ref[b, 0, :, n:n + 256] = res[b * per_img:(b + 1) * per_img]


def proj(x, tot, norm, weights, n_row, n_col, per_dev):
    n_img, n_rows, n_cols, n_chan = x.shape
    _, n_heads, hd, _ = weights.shape
    count = float(n_rows * n_cols * n_row * n_col * (n_chan // GROUPS))
    n_grp = n_heads // per_dev
    width = -(-per_dev * 3 * hd // 256) * 256
    return pl.pallas_call(
        functools.partial(proj_kernel, count, per_dev),
        grid=(n_grp,),
        out_shape=jax.ShapeDtypeStruct((n_img, n_grp, n_rows * n_cols, width), BF16),
        in_specs=[
            pl.BlockSpec(x.shape, lambda q: (0, 0, 0, 0)),
            pl.BlockSpec((8, LANES), lambda q: (0, 0)),
            pl.BlockSpec(norm.shape, lambda q: (0, 0)),
            pl.BlockSpec((3, per_dev, hd, n_chan), lambda q: (0, q, 0, 0)),
        ],
        out_specs=pl.BlockSpec((n_img, 1, n_rows * n_cols, width), lambda q: (0, q, 0, 0)),
        scratch_shapes=[pltpu.VMEM((n_img * n_rows * n_cols, n_chan), BF16), pltpu.VMEM((width, n_chan), BF16)],
        compiler_params=pltpu.CompilerParams(vmem_limit_bytes=VMEM_LIMIT),
        name="proj",
    )(x, tot, norm, weights)


def attend_kernel(hd, q_ref, kv_ref, out_ref, qt, vt, ot, qf):
    n_q, n_k = q_ref.shape[0], kv_ref.shape[0]
    half = lax.rem(pl.program_id(0), 2)
    factor = 1.4426950408889634 * hd ** -0.5
    kb, qb = min(1024, n_k), min(512, n_q)
    tb = min(512, n_q)
    for t in range(0, n_q, tb):
        qf[:, t:t + tb] = q_ref[t:t + tb, :].astype(F32).T
    qt[0:hd, :] = qf[pl.ds(pl.multiple_of(half * hd, hd), hd), :].astype(BF16)
    qt[hd:, :] = jnp.zeros((qt.shape[0] - hd, n_q), BF16)

    def flip(t, carry):
        at = pl.multiple_of(t * tb, tb)
        vt[:, pl.ds(at, tb)] = kv_ref[pl.ds(at, tb), :].astype(F32).T[hd:].astype(BF16)
        return carry

    lax.fori_loop(0, n_k // tb, flip, 0)

    def queries(t, carry):
        at = pl.multiple_of(t * qb, qb)
        rhs = qt[:, pl.ds(at, qb)]

        def keys(s, state):
            run_max, run_sum, out = state
            pos = pl.multiple_of(s * kb, kb)
            logits = jnp.dot(kv_ref[pl.ds(pos, kb), :], rhs, preferred_element_type=F32)
            new_max = jnp.maximum(run_max, jnp.max(logits, axis=0, keepdims=True))
            scale = jnp.exp2((run_max - new_max) * factor)
            w = jnp.exp2((logits - new_max) * factor)
            run_sum = run_sum * scale + jnp.sum(w, axis=0, keepdims=True)
            out = out * scale + jnp.dot(vt[:, pl.ds(pos, kb)], w.astype(BF16), preferred_element_type=F32)
            return new_max, run_sum, out

        init = (jnp.full((1, qb), -jnp.inf, F32), jnp.zeros((1, qb), F32), jnp.zeros((hd, qb), F32))
        _, run_sum, out = lax.fori_loop(0, n_k // kb, keys, init)
        ot[pl.ds(pl.multiple_of(half * hd, hd), hd), pl.ds(at, qb)] = out / run_sum
        return carry

    lax.fori_loop(0, n_q // qb, queries, 0)
    for t in range(0, n_q, tb):
        out_ref[t:t + tb, :] = ot[:, t:t + tb].T.astype(BF16)


def attend(q, kv, hd, per_dev):
    n_q, n_k = q.shape[0], kv.shape[0]
    return pl.pallas_call(
        functools.partial(attend_kernel, hd),
        grid=(per_dev,),
        out_shape=jax.ShapeDtypeStruct(q.shape, BF16),
        in_specs=[pl.BlockSpec((n_q, 2 * hd), lambda i: (0, i // 2)), pl.BlockSpec((n_k, 2 * hd), lambda i: (0, i))],
        out_specs=pl.BlockSpec((n_q, 2 * hd), lambda i: (0, i // 2)),
        scratch_shapes=[pltpu.VMEM((2 * hd, n_q), BF16), pltpu.VMEM((hd, n_k), BF16), pltpu.VMEM((2 * hd, n_q), F32), pltpu.VMEM((2 * hd, n_q), F32)],
        compiler_params=pltpu.CompilerParams(vmem_limit_bytes=VMEM_LIMIT),
        name="attend",
    )(q, kv)


def outproj_kernel(o_ref, w_ref, x_ref, out_ref, edge_ref, part_ref, wcat, acc, csum):
    n_img, n_rows, n_cols, n_chan = x_ref.shape
    per_dev, hd, _ = w_ref.shape[1:]
    per_img = n_rows * n_cols
    q = pl.program_id(0)

    @pl.when(q == 0)
    def _():
        acc[...] = x_ref[...].reshape(acc.shape).astype(F32)
        wcat[per_dev * hd:, :] = jnp.zeros((wcat.shape[0] - per_dev * hd, n_chan), BF16)

    for i in range(per_dev):
        wcat[i * hd:(i + 1) * hd, :] = w_ref[0, i]
    lhs = o_ref[:, 0].reshape(n_img * per_img, o_ref.shape[3])
    for n in range(0, n_chan, 256):
        acc[:, n:n + 256] += jnp.dot(lhs, wcat[:, n:n + 256], preferred_element_type=F32)

    @pl.when(q == pl.num_programs(0) - 1)
    def _():
        finish(acc, out_ref, edge_ref, part_ref, csum)


def outproj(o, weights, x, per_dev):
    n_img, n_grp, n_tok, width = o.shape
    _, n_heads, hd, n_chan = weights.shape
    shapes = [jax.ShapeDtypeStruct(x.shape, BF16)] + finish_shapes(x.shape)
    return pl.pallas_call(
        outproj_kernel,
        grid=(n_grp,),
        out_shape=shapes,
        in_specs=[
            pl.BlockSpec((n_img, 1, n_tok, width), lambda q: (0, q, 0, 0)),
            pl.BlockSpec((1, per_dev, hd, n_chan), lambda q: (3, q, 0, 0)),
            pl.BlockSpec(x.shape, lambda q: (0, 0, 0, 0)),
        ],
        out_specs=[pl.BlockSpec(s.shape, lambda q, n=len(s.shape): (0,) * n) for s in shapes],
        scratch_shapes=[pltpu.VMEM((width, n_chan), BF16), pltpu.VMEM((n_img * n_tok, n_chan), F32), pltpu.VMEM((8, n_chan), F32)],
        compiler_params=pltpu.CompilerParams(vmem_limit_bytes=VMEM_LIMIT),
        name="outproj",
    )(o, weights, x)


def solution(mesh):
    n_row, n_col = mesh.shape['row'], mesh.shape['col']

    def res_block(blk, x, edge, part, t_emb, res_norm, res_conv, res_temb):
        t_act = jax.nn.silu(t_emb.astype(F32)).astype(BF16)
        t_proj = jnp.dot(t_act, res_temb[blk], preferred_element_type=F32)
        halos = exchange(part, n_row, n_col, x, edge)
        h, edge, part = conv(blk, 0, x, halos, res_norm, t_proj, res_conv, n_row, n_col, False)
        halos = exchange(part, n_row, n_col, h, edge)
        return conv(blk, 1, h, halos, res_norm, x, res_conv, n_row, n_col, True)

    def attn_block(x, part, norm, weights):
        n_img, n_rows, n_cols, n_chan = x.shape
        weights = jnp.swapaxes(weights, 2, 3)
        n_heads, hd = weights.shape[1], weights.shape[2]
        per_dev = n_img * n_heads // n_row
        n_tok = n_rows * n_cols
        tot, = exchange(part, n_row, n_col)
        qkv = proj(x, tot, norm, weights, n_row, n_col, per_dev)
        qkv = lax.all_to_all(qkv.reshape(n_row, n_tok, -1), 'row', 0, 0).reshape(n_row * n_tok, -1)
        kv_width = per_dev * 2 * hd
        q_width = -(-per_dev // 2) * 2 * hd
        kv = lax.all_gather(qkv[:, :kv_width], 'col', axis=0, tiled=True)
        out = attend(qkv[:, kv_width:kv_width + q_width], kv, hd, per_dev)
        out = lax.all_to_all(out.reshape(n_row, n_tok, q_width), 'row', 0, 0)
        return outproj(out.reshape(n_img, -1, n_tok, q_width), weights, x, per_dev)

    def run_stage(latent, t_emb, res_norm, res_conv, res_temb, attn_norm, attn_proj):
        edge, part = prep(latent)
        x, edge, part = res_block(0, latent, edge, part, t_emb, res_norm, res_conv, res_temb)
        x, edge, part = attn_block(x, part, attn_norm, attn_proj)
        return res_block(1, x, edge, part, t_emb, res_norm, res_conv, res_temb)[0]

    spec_x = P('dp', 'row', 'col', None)
    return jax.shard_map(run_stage, mesh=mesh, in_specs=(spec_x, P('dp', None), P(), P(), P(), P(), P()), out_specs=spec_x, check_vma=False)
```

```python
import functools

import jax
import jax.numpy as jnp
from jax import lax
from jax.experimental import pallas as pl
from jax.experimental.pallas import tpu as pltpu
from jax.sharding import PartitionSpec as P

GROUPS = 32
EPS = 1e-5
LANES = 128
ROOM = 60.0
TINY = 2.0 ** -90
MESH = pl.DeviceIdType.MESH
HIGH = lax.Precision.HIGHEST
F32 = jnp.float32
BF16 = jnp.bfloat16
VMEM_LIMIT = 60 * 1024 * 1024
VSPEC = pl.BlockSpec(memory_space=pltpu.VMEM)
ASPEC = pl.BlockSpec(memory_space=pl.ANY)


def group_mask(n_chan, chan_axis):
    width = n_chan // GROUPS
    shape = (n_chan, LANES) if chan_axis == 0 else (LANES, n_chan)
    chan = lax.broadcasted_iota(jnp.int32, shape, chan_axis)
    first = lax.broadcasted_iota(jnp.int32, shape, 1 - chan_axis) * width
    return jnp.where((chan >= first) & (chan < first + width), 1.0, 0.0).astype(F32)


def channel_stats(tot, count):
    vals = tot / count
    mean = vals[0:2]
    inv = lax.rsqrt(vals[2:4] - mean * mean + EPS)
    return jnp.concatenate([mean, inv, jnp.zeros((4, LANES), F32)], axis=0)


def expand(stats, n_chan):
    return jnp.dot(stats, group_mask(n_chan, 1), precision=HIGH, preferred_element_type=F32)


def silu(u):
    half = 0.5 * u
    return half * jnp.tanh(half) + half


def finish(acc, out_ref, edge_ref, part_ref, csum):
    n_img, n_rows, n_cols, n_chan = out_ref.shape
    per_img = n_rows * n_cols
    csum[...] = jnp.zeros_like(csum)
    for ch in range(0, n_chan, 256):
        sl = slice(ch, ch + 256)
        for b in range(n_img):
            val = acc[b * per_img:(b + 1) * per_img, sl].astype(BF16)
            out_ref[b, :, :, sl] = val.reshape(n_rows, n_cols, 256)
            val = val.astype(F32)
            csum[b:b + 1, sl] = jnp.sum(val, axis=0, keepdims=True)
            csum[2 + b:3 + b, sl] = jnp.sum(val * val, axis=0, keepdims=True)
    for side, col in ((0, 0), (1, n_cols - 1)):
        for i in range(n_rows):
            rows = [acc[b * per_img + i * n_cols + col:b * per_img + i * n_cols + col + 1, :] for b in range(n_img)]
            edge_ref[side, i] = jnp.concatenate(rows, axis=0).astype(BF16)
    part_ref[...] = jnp.dot(csum[...], group_mask(n_chan, 0), precision=HIGH, preferred_element_type=F32)


def prep_kernel(x_ref, edge_ref, part_ref, acc, dump, csum):
    n_img, n_rows, n_cols, n_chan = x_ref.shape
    acc[...] = x_ref[...].reshape(acc.shape).astype(F32)
    finish(acc, dump, edge_ref, part_ref, csum)


def finish_shapes(shape):
    n_img, n_rows, n_cols, n_chan = shape
    return [jax.ShapeDtypeStruct((2, n_rows, n_img, n_chan), BF16), jax.ShapeDtypeStruct((8, LANES), F32)]


def prep(x):
    n_tok = x.shape[0] * x.shape[1] * x.shape[2]
    return pl.pallas_call(
        prep_kernel,
        out_shape=finish_shapes(x.shape),
        in_specs=[VSPEC],
        out_specs=[VSPEC, VSPEC],
        scratch_shapes=[pltpu.VMEM((n_tok, x.shape[3]), F32), pltpu.VMEM(x.shape, BF16), pltpu.VMEM((8, x.shape[3]), F32)],
        compiler_params=pltpu.CompilerParams(vmem_limit_bytes=VMEM_LIMIT),
        name="prep",
    )(x)


def exchange_kernel(n_row, n_col, halo, *refs):
    if halo:
        part_ref, x_ref, edge_ref, tot_ref, top_ref, bot_ref, side_ref, buf, send, recv = refs
    else:
        part_ref, tot_ref, buf, send, recv = refs
    r, c = lax.axis_index('row'), lax.axis_index('col')
    up, down = lax.rem(r + n_row - 1, n_row), lax.rem(r + 1, n_row)
    left, right = lax.rem(c + n_col - 1, n_col), lax.rem(c + 1, n_col)
    peers = [{'row': lax.rem(r + i, n_row), 'col': lax.rem(c + j, n_col)} for i in range(n_row) for j in range(n_col) if i or j]
    barrier = pltpu.get_barrier_semaphore()
    for peer in peers:
        pl.semaphore_signal(barrier, inc=1, device_id=peer, device_id_type=MESH)
    pl.semaphore_wait(barrier, len(peers))

    def copy(src, dst, slot, peer):
        return pltpu.make_async_remote_copy(src_ref=src, dst_ref=dst, send_sem=send.at[slot], recv_sem=recv.at[slot], device_id=peer, device_id_type=MESH)

    copies = [copy(part_ref, buf.at[k], k, peer) for k, peer in enumerate(peers)]
    for cp in copies:
        cp.start()
    halos = []
    if halo:
        last = x_ref.shape[1] - 1
        end = side_ref.shape[1] - 1
        plan = [
            (x_ref.at[:, last], top_ref, {'row': down}),
            (x_ref.at[:, 0], bot_ref, {'row': up}),
            (edge_ref.at[0], side_ref.at[1, 1:end], {'col': left}),
            (edge_ref.at[1], side_ref.at[0, 1:end], {'col': right}),
            (edge_ref.at[0, 0], side_ref.at[1, end], {'row': up, 'col': left}),
            (edge_ref.at[0, last], side_ref.at[1, 0], {'row': down, 'col': left}),
            (edge_ref.at[1, 0], side_ref.at[0, end], {'row': up, 'col': right}),
            (edge_ref.at[1, last], side_ref.at[0, 0], {'row': down, 'col': right}),
        ]
        halos = [copy(src, dst, len(peers) + i, peer) for i, (src, dst, peer) in enumerate(plan)]
        for cp in halos:
            cp.start()
    total = part_ref[...]
    for k, cp in enumerate(copies):
        cp.wait_recv()
        total = total + buf[k]
    tot_ref[...] = total
    for cp in halos:
        cp.wait_recv()
    for cp in copies + halos:
        cp.wait_send()


def exchange(part, n_row, n_col, x=None, edge=None):
    halo = x is not None
    out_shape = [jax.ShapeDtypeStruct((8, LANES), F32)]
    args = [part]
    in_specs = [VSPEC]
    if halo:
        n_img, n_rows, n_cols, n_chan = x.shape
        out_shape += [
            jax.ShapeDtypeStruct((n_img, n_cols, n_chan), BF16),
            jax.ShapeDtypeStruct((n_img, n_cols, n_chan), BF16),
            jax.ShapeDtypeStruct((2, n_rows + 2, n_img, n_chan), BF16),
        ]
        args += [x, edge]
        in_specs += [ASPEC, VSPEC]
    n_peer = n_row * n_col - 1
    n_sem = n_peer + (8 if halo else 0)
    return pl.pallas_call(
        functools.partial(exchange_kernel, n_row, n_col, halo),
        out_shape=out_shape,
        in_specs=in_specs,
        out_specs=[VSPEC] + [ASPEC] * (len(out_shape) - 1),
        scratch_shapes=[
            pltpu.VMEM((n_peer, 8, LANES), F32),
            pltpu.SemaphoreType.DMA((n_sem,)),
            pltpu.SemaphoreType.DMA((n_sem,)),
        ],
        compiler_params=pltpu.CompilerParams(collective_id=1 if halo else 2, has_side_effects=True, vmem_limit_bytes=VMEM_LIMIT),
        name="exchange",
    )(*args)


def conv_kernel(blk, idx, n_row, n_col, count, residual, x_ref, top_ref, bot_ref, side_ref, tot_ref, norm_ref, add_ref, w_hbm,
                out_ref, edge_ref, part_ref, act, hside, stat, wbuf, acc, csum, sem):
    n_img, n_rows, n_cols, n_chan = x_ref.shape
    per_img = n_rows * n_cols

    def fetch(dy):
        return pltpu.make_async_copy(w_hbm.at[blk, idx, dy], wbuf.at[dy], sem.at[dy])

    for dy in range(3):
        fetch(dy).start()
    r, c = lax.axis_index('row'), lax.axis_index('col')
    st = expand(channel_stats(tot_ref[...], count), n_chan)
    gain = norm_ref[blk, idx, 0:1, :].astype(F32)
    shift = norm_ref[blk, idx, 1:2, :].astype(F32)
    stat[0:2] = st[0:2]
    stat[2:4] = st[2:4] * gain
    stat[4:5] = shift

    for side in range(2):
        inside = (c > 0) if side == 0 else (c < n_col - 1)
        for i in range(n_rows + 2):
            ok = inside
            if i == 0:
                ok = ok & (r > 0)
            if i == n_rows + 1:
                ok = ok & (r < n_row - 1)
            z = side_ref[side, i].astype(F32)
            a = silu((z - stat[0:2]) * stat[2:4] + stat[4:5])
            hside[side, i] = jnp.where(ok, a, 0.0)

    step = 256

    def place(b, i, src, ok):
        rows = lax.broadcasted_iota(jnp.int32, (n_cols, step), 0)
        for ch in range(0, n_chan, step):
            sl = slice(ch, ch + step)
            z = src(sl).astype(F32)
            a = silu((z - stat[b:b + 1, sl]) * stat[2 + b:3 + b, sl] + stat[4:5, sl])
            if ok is not None:
                a = jnp.where(ok, a, 0.0)
            act[b, i, :, n_chan + ch:n_chan + ch + step] = a.astype(BF16)
            lo = jnp.where(rows == 0, hside[0, i, b:b + 1, sl], pltpu.roll(a, 1, 0))
            act[b, i, :, ch:ch + step] = lo.astype(BF16)
            hi = jnp.where(rows == n_cols - 1, hside[1, i, b:b + 1, sl], pltpu.roll(a, n_cols - 1, 0))
            act[b, i, :, 2 * n_chan + ch:2 * n_chan + ch + step] = hi.astype(BF16)

    for b in range(n_img):
        place(b, 0, lambda sl, b=b: top_ref[b, :, sl], r > 0)

        def middle(i, carry, b=b):
            place(b, i + 1, lambda sl: x_ref[b, i, :, sl], None)
            return carry

        lax.fori_loop(0, n_rows, middle, 0)
        place(b, n_rows + 1, lambda sl, b=b: bot_ref[b, :, sl], r < n_row - 1)

    if residual:
        acc[...] = add_ref[...].reshape(acc.shape).astype(F32)
    else:
        for b in range(n_img):
            acc[b * per_img:(b + 1) * per_img, :] = jnp.broadcast_to(add_ref[b:b + 1, :], (per_img, n_chan))

    def taps(dy, carry):
        fetch(dy).wait()
        lhs = act[:, pl.ds(dy, n_rows)].reshape(n_img * per_img, 3 * n_chan)
        for ch in range(0, n_chan, 256):
            rhs = wbuf[dy, :, :, ch:ch + 256].reshape(3 * n_chan, 256)
            acc[:, ch:ch + 256] += jnp.dot(lhs, rhs, preferred_element_type=F32)
        return carry

    lax.fori_loop(0, 3, taps, 0)
    finish(acc, out_ref, edge_ref, part_ref, csum)


def conv(blk, idx, x, halos, norm, add, weights, n_row, n_col, residual):
    tot, top, bot, side = halos
    n_img, n_rows, n_cols, n_chan = x.shape
    count = float(n_rows * n_cols * n_row * n_col * (n_chan // GROUPS))
    n_tok = n_img * n_rows * n_cols
    return pl.pallas_call(
        functools.partial(conv_kernel, blk, idx, n_row, n_col, count, residual),
        out_shape=[jax.ShapeDtypeStruct(x.shape, BF16)] + finish_shapes(x.shape),
        in_specs=[VSPEC] * 7 + [ASPEC],
        out_specs=[VSPEC] * 3,
        scratch_shapes=[
            pltpu.VMEM((n_img, n_rows + 2, n_cols, 3 * n_chan), BF16),
            pltpu.VMEM((2, n_rows + 2, n_img, n_chan), F32),
            pltpu.VMEM((8, n_chan), F32),
            pltpu.VMEM((3, 3, n_chan, n_chan), BF16),
            pltpu.VMEM((n_tok, n_chan), F32),
            pltpu.VMEM((8, n_chan), F32),
            pltpu.SemaphoreType.DMA((3,)),
        ],
        compiler_params=pltpu.CompilerParams(vmem_limit_bytes=VMEM_LIMIT),
        cost_estimate=pl.CostEstimate(flops=2 * 9 * n_tok * n_chan * n_chan, bytes_accessed=9 * 2 * n_chan * n_chan, transcendentals=n_tok * n_chan),
        name="conv",
    )(x, top, bot, side, tot, norm, add, weights)


def head_blocks(per_dev):
    return [(i, min(2, per_dev - i)) for i in range(0, per_dev, 2)]


def proj_kernel(count, per_dev, x_ref, tot_ref, norm_ref, w_ref, *refs):
    n_img, n_rows, n_cols, n_chan = x_ref.shape
    per_img = n_rows * n_cols
    hd = w_ref.shape[2]
    blocks = head_blocks(per_dev)
    outs, g, wcat = refs[:len(blocks)], refs[-2], refs[-1]

    @pl.when(pl.program_id(0) == 0)
    def _():
        st = expand(channel_stats(tot_ref[...], count), n_chan)
        gain = norm_ref[0:1, :].astype(F32)
        shift = norm_ref[1:2, :].astype(F32)
        for b in range(n_img):
            z = x_ref[b].reshape(per_img, n_chan).astype(F32)
            g[b * per_img:(b + 1) * per_img, :] = ((z - st[b:b + 1]) * (st[2 + b:3 + b] * gain) + shift).astype(BF16)

    for (first, n), out_ref in zip(blocks, outs):
        for i in range(n):
            wcat[2 * i * hd:(2 * i + 1) * hd, :] = w_ref[1, first + i]
            wcat[(2 * i + 1) * hd:(2 * i + 2) * hd, :] = w_ref[2, first + i]
            wcat[(2 * n + i) * hd:(2 * n + i + 1) * hd, :] = w_ref[0, first + i]
        width = out_ref.shape[3]
        if n == 1:
            wcat[3 * hd:width, :] = jnp.zeros((width - 3 * hd, n_chan), BF16)
        res = lax.dot_general(g[...], wcat[0:width, :], (((1,), (1,)), ((), ())), preferred_element_type=F32).astype(BF16)
        for b in range(n_img):
            out_ref[b, 0] = res[b * per_img:(b + 1) * per_img]


def proj(x, tot, norm, weights, n_row, n_col, per_dev):
    n_img, n_rows, n_cols, n_chan = x.shape
    _, n_heads, hd, _ = weights.shape
    count = float(n_rows * n_cols * n_row * n_col * (n_chan // GROUPS))
    n_grp = n_heads // per_dev
    n_tok = n_rows * n_cols
    widths = [2 * hd * (n + 1) for _, n in head_blocks(per_dev)]
    return pl.pallas_call(
        functools.partial(proj_kernel, count, per_dev),
        grid=(n_grp,),
        out_shape=[jax.ShapeDtypeStruct((n_img, n_grp, n_tok, w), BF16) for w in widths],
        in_specs=[
            pl.BlockSpec(x.shape, lambda q: (0, 0, 0, 0)),
            pl.BlockSpec((8, LANES), lambda q: (0, 0)),
            pl.BlockSpec(norm.shape, lambda q: (0, 0)),
            pl.BlockSpec((3, per_dev, hd, n_chan), lambda q: (0, q, 0, 0)),
        ],
        out_specs=[pl.BlockSpec((n_img, 1, n_tok, w), lambda q: (0, q, 0, 0)) for w in widths],
        scratch_shapes=[pltpu.VMEM((n_img * n_tok, n_chan), BF16), pltpu.VMEM((max(widths), n_chan), BF16)],
        compiler_params=pltpu.CompilerParams(vmem_limit_bytes=VMEM_LIMIT),
        cost_estimate=pl.CostEstimate(flops=2 * n_img * n_tok * n_chan * n_grp * sum(widths), bytes_accessed=6 * n_chan * n_chan, transcendentals=0),
        name="proj",
    )(x, tot, norm, weights)


def attend_kernel(hd, n_pair, q_ref, kv_ref, out_ref, qt, qf, kk, vt, ot, w0, w1, osum, lsum, big):
    n_q, n_k = q_ref.shape[0], kv_ref.shape[0]
    half = pl.multiple_of(pl.program_id(0) * hd, hd)
    factor = 1.4426950408889634 * hd ** -0.5
    kb, qb = w0.shape
    tb = min(512, n_q)

    @pl.when(pl.program_id(0) == 0)
    def _():
        lane = lax.broadcasted_iota(jnp.int32, (n_k, 2 * hd), 1)
        kk[:, 2 * hd:] = jnp.where(lane == 0, 1.0, 0.0).astype(BF16)
        if n_pair == 1:
            ot[hd:, :] = jnp.zeros((hd, n_q), F32)

    def flip(t, top):
        at = pl.multiple_of(t * tb, tb)
        blk = kv_ref[pl.ds(at, tb), :].astype(F32)
        turned = blk.T
        vt[:, pl.ds(at, tb)] = turned[hd:].astype(BF16)
        lane = lax.broadcasted_iota(jnp.int32, blk.shape, 1)
        kk[pl.ds(at, tb), 0:2 * hd] = jnp.where(lane < hd, blk, pltpu.roll(blk, hd, 1)).astype(BF16)
        return jnp.maximum(top, jnp.sum(turned[:hd] * turned[:hd], axis=0, keepdims=True))

    top = lax.fori_loop(0, n_k // tb, flip, jnp.zeros((1, tb), F32))
    key_norm = jnp.sqrt(jnp.max(top, axis=1, keepdims=True))

    for t in range(0, n_q, tb):
        qf[:, t:t + tb] = q_ref[t:t + tb, :].astype(F32).T
    scaled = qf[pl.ds(half, hd), :] * factor
    high = scaled.astype(BF16)
    qt[0:hd, :] = high
    qt[hd:2 * hd, :] = (scaled - high.astype(F32)).astype(BF16)
    bound = jnp.sqrt(jnp.sum(scaled * scaled, axis=0, keepdims=True)) * key_norm
    row = lax.broadcasted_iota(jnp.int32, (2 * hd, n_q), 0)
    qt[2 * hd:, :] = jnp.where(row == 0, ROOM - bound, 0.0).astype(BF16)

    n_blk = n_k // kb

    def queries(t, carry):
        at = pl.multiple_of(t * qb, qb)
        rhs = qt[:, pl.ds(at, qb)]

        def weigh(s, dst):
            pos = pl.multiple_of(s * kb, kb)
            w = jnp.exp2(jnp.dot(kk[pl.ds(pos, kb), :], rhs, preferred_element_type=F32))
            dst[...] = w.astype(BF16)
            return jnp.sum(w.reshape(kb // 8, 8, qb), axis=0)

        def gather(s, src):
            pos = pl.multiple_of(s * kb, kb)
            osum[...] += jnp.dot(vt[:, pl.ds(pos, kb)], src[...], preferred_element_type=F32)

        osum[...] = jnp.zeros_like(osum)
        total = weigh(0, w0)

        def keys(j, total):
            total += weigh(2 * j + 1, w1)
            gather(2 * j, w0)
            total += weigh(2 * j + 2, w0)
            gather(2 * j + 1, w1)
            return total

        total = lax.fori_loop(0, n_blk // 2 - 1, keys, total)
        total += weigh(n_blk - 1, w1)
        gather(n_blk - 2, w0)
        gather(n_blk - 1, w1)
        total = jnp.sum(total, axis=0, keepdims=True)
        lsum[:, pl.ds(at, qb)] = total
        big[:, pl.ds(at, qb)] = jnp.max(jnp.abs(osum[...]), axis=0, keepdims=True)
        ot[pl.ds(half, hd), pl.ds(at, qb)] = osum[...] / total
        return carry

    lax.fori_loop(0, n_q // qb, queries, 0)
    sound = (jnp.min(lsum[...]) >= TINY) & (jnp.max(big[...]) <= 3e38) & (jnp.max(lsum[...]) <= 3e38)

    @pl.when(jnp.logical_not(sound))
    def _():
        qt[2 * hd:, :] = jnp.zeros((2 * hd, n_q), BF16)
        sk, sq = min(256, n_k), min(256, n_q)

        def some_queries(t, carry):
            at = pl.multiple_of(t * sq, sq)

            def some_keys(s, state):
                run_max, run_sum, out = state
                pos = pl.multiple_of(s * sk, sk)
                logits = jnp.dot(kk[pl.ds(pos, sk), :], qt[:, pl.ds(at, sq)], preferred_element_type=F32)
                new_max = jnp.maximum(run_max, jnp.max(logits, axis=0, keepdims=True))
                scale = jnp.exp2(run_max - new_max)
                w = jnp.exp2(logits - new_max)
                run_sum = run_sum * scale + jnp.sum(w, axis=0, keepdims=True)
                out = out * scale + jnp.dot(vt[:, pl.ds(pos, sk)], w.astype(BF16), preferred_element_type=F32)
                return new_max, run_sum, out

            init = (jnp.full((1, sq), -jnp.inf, F32), jnp.zeros((1, sq), F32), jnp.zeros((hd, sq), F32))
            _, run_sum, out = lax.fori_loop(0, n_k // sk, some_keys, init)
            ot[pl.ds(half, hd), pl.ds(at, sq)] = out / run_sum
            return carry

        lax.fori_loop(0, n_q // sq, some_queries, 0)

    for t in range(0, n_q, tb):
        out_ref[t:t + tb, :] = ot[:, t:t + tb].T.astype(BF16)


def attend(q, kv, hd, n_pair, kb=1024, qb=768):
    n_q, n_k = q.shape[0], kv.shape[0]
    kb, qb = min(kb, n_k // 2), min(qb, n_q)
    return pl.pallas_call(
        functools.partial(attend_kernel, hd, n_pair),
        grid=(n_pair,),
        out_shape=jax.ShapeDtypeStruct(q.shape, BF16),
        in_specs=[pl.BlockSpec((n_q, 2 * hd), lambda i: (0, 0)), pl.BlockSpec((n_k, 2 * hd), lambda i: (0, i))],
        out_specs=pl.BlockSpec((n_q, 2 * hd), lambda i: (0, 0)),
        scratch_shapes=[
            pltpu.VMEM((4 * hd, n_q), BF16),
            pltpu.VMEM((2 * hd, n_q), F32),
            pltpu.VMEM((n_k, 4 * hd), BF16),
            pltpu.VMEM((hd, n_k), BF16),
            pltpu.VMEM((2 * hd, n_q), F32),
            pltpu.VMEM((kb, qb), BF16),
            pltpu.VMEM((kb, qb), BF16),
            pltpu.VMEM((hd, qb), F32),
            pltpu.VMEM((1, n_q), F32),
            pltpu.VMEM((1, n_q), F32),
        ],
        compiler_params=pltpu.CompilerParams(vmem_limit_bytes=VMEM_LIMIT),
        cost_estimate=pl.CostEstimate(flops=16 * n_pair * n_q * n_k * hd, bytes_accessed=n_pair * n_k * hd * 4, transcendentals=n_pair * n_q * n_k),
        name="attend",
    )(q, kv)


def outproj_kernel(n_in, *refs):
    o_refs = refs[:n_in]
    w_ref, x_ref, out_ref, edge_ref, part_ref, wcat, acc, csum = refs[n_in:]
    n_img, n_rows, n_cols, n_chan = x_ref.shape
    per_dev, hd, _ = w_ref.shape[1:]
    per_img = n_rows * n_cols
    q = pl.program_id(0)

    @pl.when(q == 0)
    def _():
        acc[...] = x_ref[...].reshape(acc.shape).astype(F32)
        wcat[per_dev * hd:, :] = jnp.zeros((wcat.shape[0] - per_dev * hd, n_chan), BF16)

    for i in range(per_dev):
        wcat[i * hd:(i + 1) * hd, :] = w_ref[0, i]
    lhs = jnp.concatenate([o[:, 0].reshape(n_img * per_img, o.shape[3]) for o in o_refs], axis=1)
    for n in range(0, n_chan, 256):
        acc[:, n:n + 256] += jnp.dot(lhs, wcat[:, n:n + 256], preferred_element_type=F32)

    @pl.when(q == pl.num_programs(0) - 1)
    def _():
        finish(acc, out_ref, edge_ref, part_ref, csum)


def outproj(outs, weights, x, per_dev):
    n_img, n_grp, n_tok, width = outs[0].shape
    _, n_heads, hd, n_chan = weights.shape
    shapes = [jax.ShapeDtypeStruct(x.shape, BF16)] + finish_shapes(x.shape)
    return pl.pallas_call(
        functools.partial(outproj_kernel, len(outs)),
        grid=(n_grp,),
        out_shape=shapes,
        in_specs=[pl.BlockSpec((n_img, 1, n_tok, width), lambda q: (0, q, 0, 0)) for _ in outs] + [
            pl.BlockSpec((1, per_dev, hd, n_chan), lambda q: (3, q, 0, 0)),
            pl.BlockSpec(x.shape, lambda q: (0, 0, 0, 0)),
        ],
        out_specs=[pl.BlockSpec(s.shape, lambda q, n=len(s.shape): (0,) * n) for s in shapes],
        scratch_shapes=[pltpu.VMEM((len(outs) * width, n_chan), BF16), pltpu.VMEM((n_img * n_tok, n_chan), F32), pltpu.VMEM((8, n_chan), F32)],
        compiler_params=pltpu.CompilerParams(vmem_limit_bytes=VMEM_LIMIT),
        cost_estimate=pl.CostEstimate(flops=2 * n_img * n_tok * n_chan * n_chan, bytes_accessed=2 * n_chan * n_chan, transcendentals=0),
        name="outproj",
    )(*outs, weights, x)


def solution(mesh):
    n_row, n_col = mesh.shape['row'], mesh.shape['col']

    def res_block(blk, x, edge, part, t_emb, res_norm, res_conv, res_temb):
        t_act = jax.nn.silu(t_emb.astype(F32)).astype(BF16)
        t_proj = jnp.dot(t_act, res_temb[blk], preferred_element_type=F32)
        halos = exchange(part, n_row, n_col, x, edge)
        h, edge, part = conv(blk, 0, x, halos, res_norm, t_proj, res_conv, n_row, n_col, False)
        halos = exchange(part, n_row, n_col, h, edge)
        return conv(blk, 1, h, halos, res_norm, x, res_conv, n_row, n_col, True)

    def attn_block(x, part, norm, weights):
        n_img, n_rows, n_cols, n_chan = x.shape
        weights = jnp.swapaxes(weights, 2, 3)
        n_heads, hd = weights.shape[1], weights.shape[2]
        per_dev = n_img * n_heads // n_row
        n_tok = n_rows * n_cols
        tot, = exchange(part, n_row, n_col)
        qkv = proj(x, tot, norm, weights, n_row, n_col, per_dev)
        blocks = head_blocks(per_dev)
        outs = [None] * len(blocks)
        for k in sorted(range(len(blocks)), key=lambda k: blocks[k][1]):
            n_pair = blocks[k][1]
            kv_width = n_pair * 2 * hd
            mine = lax.all_to_all(qkv[k].reshape(n_row, n_tok, -1), 'row', 0, 0).reshape(n_row * n_tok, -1)
            kv = lax.all_gather(mine[:, :kv_width], 'col', axis=0, tiled=True)
            out = attend(mine[:, kv_width:], kv, hd, n_pair)
            out = lax.all_to_all(out.reshape(n_row, n_tok, 2 * hd), 'row', 0, 0)
            outs[k] = out.reshape(n_img, -1, n_tok, 2 * hd)
        return outproj(outs, weights, x, per_dev)

    def run_stage(latent, t_emb, res_norm, res_conv, res_temb, attn_norm, attn_proj):
        edge, part = prep(latent)
        x, edge, part = res_block(0, latent, edge, part, t_emb, res_norm, res_conv, res_temb)
        x, edge, part = attn_block(x, part, attn_norm, attn_proj)
        return res_block(1, x, edge, part, t_emb, res_norm, res_conv, res_temb)[0]

    spec_x = P('dp', 'row', 'col', None)
    return jax.shard_map(run_stage, mesh=mesh, in_specs=(spec_x, P('dp', None), P(), P(), P(), P(), P()), out_specs=spec_x, check_vma=False)
```

```python
import functools

import jax
import jax.numpy as jnp
from jax import lax
from jax.experimental import pallas as pl
from jax.experimental.pallas import tpu as pltpu
from jax.sharding import PartitionSpec as P

GROUPS = 32
EPS = 1e-5
LANES = 128
ROOM = 60.0
TINY = 2.0 ** -90
MESH = pl.DeviceIdType.MESH
HIGH = lax.Precision.HIGHEST
F32 = jnp.float32
BF16 = jnp.bfloat16
VMEM_LIMIT = 60 * 1024 * 1024
VSPEC = pl.BlockSpec(memory_space=pltpu.VMEM)
ASPEC = pl.BlockSpec(memory_space=pl.ANY)


def group_mask(n_chan, chan_axis):
    width = n_chan // GROUPS
    shape = (n_chan, LANES) if chan_axis == 0 else (LANES, n_chan)
    chan = lax.broadcasted_iota(jnp.int32, shape, chan_axis)
    first = lax.broadcasted_iota(jnp.int32, shape, 1 - chan_axis) * width
    return jnp.where((chan >= first) & (chan < first + width), 1.0, 0.0).astype(F32)


def channel_stats(tot, count):
    vals = tot / count
    mean = vals[0:2]
    inv = lax.rsqrt(vals[2:4] - mean * mean + EPS)
    return jnp.concatenate([mean, inv, jnp.zeros((4, LANES), F32)], axis=0)


def expand(stats, n_chan):
    return jnp.dot(stats, group_mask(n_chan, 1), precision=HIGH, preferred_element_type=F32)


def silu(u):
    half = 0.5 * u
    return half * jnp.tanh(half) + half


def finish(acc, out_ref, edge_ref, part_ref, csum):
    n_img, n_rows, n_cols, n_chan = out_ref.shape
    per_img = n_rows * n_cols
    csum[...] = jnp.zeros_like(csum)
    for ch in range(0, n_chan, 256):
        sl = slice(ch, ch + 256)
        for b in range(n_img):
            val = acc[b * per_img:(b + 1) * per_img, sl].astype(BF16)
            out_ref[b, :, :, sl] = val.reshape(n_rows, n_cols, 256)
            val = val.astype(F32)
            csum[b:b + 1, sl] = jnp.sum(val, axis=0, keepdims=True)
            csum[2 + b:3 + b, sl] = jnp.sum(val * val, axis=0, keepdims=True)
    for side, col in ((0, 0), (1, n_cols - 1)):
        for i in range(n_rows):
            rows = [acc[b * per_img + i * n_cols + col:b * per_img + i * n_cols + col + 1, :] for b in range(n_img)]
            edge_ref[side, i] = jnp.concatenate(rows, axis=0).astype(BF16)
    part_ref[...] = jnp.dot(csum[...], group_mask(n_chan, 0), precision=HIGH, preferred_element_type=F32)


def prep_kernel(x_ref, emb_ref, w_hbm, edge_ref, part_ref, t_ref, acc, dump, csum, wbuf, sem):
    n_blk = w_hbm.shape[0]
    loads = [pltpu.make_async_copy(w_hbm.at[k], wbuf.at[k], sem.at[k]) for k in range(n_blk)]
    for cp in loads:
        cp.start()
    acc[...] = x_ref[...].reshape(acc.shape).astype(F32)
    finish(acc, dump, edge_ref, part_ref, csum)
    emb = silu(emb_ref[...].astype(F32))
    n_img = emb.shape[0]
    emb = jnp.concatenate([emb, jnp.zeros((8 - n_img, emb.shape[1]), F32)], axis=0).astype(BF16)
    for k, cp in enumerate(loads):
        cp.wait()
        t_ref[k] = jnp.dot(emb, wbuf[k], preferred_element_type=F32)[0:n_img]


def finish_shapes(shape):
    n_img, n_rows, n_cols, n_chan = shape
    return [jax.ShapeDtypeStruct((2, n_rows, n_img, n_chan), BF16), jax.ShapeDtypeStruct((8, LANES), F32)]


def prep(x, t_emb, w_temb):
    n_img, n_rows, n_cols, n_chan = x.shape
    return pl.pallas_call(
        prep_kernel,
        out_shape=finish_shapes(x.shape) + [jax.ShapeDtypeStruct((w_temb.shape[0], n_img, n_chan), F32)],
        in_specs=[VSPEC, VSPEC, ASPEC],
        out_specs=[VSPEC, VSPEC, VSPEC],
        scratch_shapes=[
            pltpu.VMEM((n_img * n_rows * n_cols, n_chan), F32),
            pltpu.VMEM(x.shape, BF16),
            pltpu.VMEM((8, n_chan), F32),
            pltpu.VMEM(w_temb.shape, BF16),
            pltpu.SemaphoreType.DMA((w_temb.shape[0],)),
        ],
        compiler_params=pltpu.CompilerParams(vmem_limit_bytes=VMEM_LIMIT),
        name="prep",
    )(x, t_emb, w_temb)


def exchange_kernel(n_row, n_col, halo, *refs):
    if halo:
        part_ref, x_ref, edge_ref, tot_ref, top_ref, bot_ref, side_ref, rbuf, cbuf, rsum, send, recv = refs
    else:
        part_ref, tot_ref, rbuf, cbuf, rsum, send, recv = refs
    r, c = lax.axis_index('row'), lax.axis_index('col')
    up, down = lax.rem(r + n_row - 1, n_row), lax.rem(r + 1, n_row)
    left, right = lax.rem(c + n_col - 1, n_col), lax.rem(c + 1, n_col)
    row_peers = [{'row': lax.rem(r + k, n_row)} for k in range(1, n_row)]
    col_peers = [{'col': lax.rem(c + k, n_col)} for k in range(1, n_col)]
    diag = [{'row': a, 'col': b} for a in (up, down) for b in (left, right)] if halo else []
    peers = row_peers + col_peers + diag
    barrier = pltpu.get_barrier_semaphore()
    for peer in peers:
        pl.semaphore_signal(barrier, inc=1, device_id=peer, device_id_type=MESH)
    pl.semaphore_wait(barrier, len(peers))

    def copy(src, dst, slot, peer):
        return pltpu.make_async_remote_copy(src_ref=src, dst_ref=dst, send_sem=send.at[slot], recv_sem=recv.at[slot], device_id=peer, device_id_type=MESH)

    first = [copy(part_ref, rbuf.at[k], k, peer) for k, peer in enumerate(row_peers)]
    for cp in first:
        cp.start()
    halos = []
    if halo:
        last = x_ref.shape[1] - 1
        end = side_ref.shape[1] - 1
        plan = [
            (x_ref.at[:, last], top_ref, {'row': down}),
            (x_ref.at[:, 0], bot_ref, {'row': up}),
            (edge_ref.at[0], side_ref.at[1, 1:end], {'col': left}),
            (edge_ref.at[1], side_ref.at[0, 1:end], {'col': right}),
            (edge_ref.at[0, 0], side_ref.at[1, end], {'row': up, 'col': left}),
            (edge_ref.at[0, last], side_ref.at[1, 0], {'row': down, 'col': left}),
            (edge_ref.at[1, 0], side_ref.at[0, end], {'row': up, 'col': right}),
            (edge_ref.at[1, last], side_ref.at[0, 0], {'row': down, 'col': right}),
        ]
        halos = [copy(src, dst, n_row + n_col - 2 + i, peer) for i, (src, dst, peer) in enumerate(plan)]
        for cp in halos:
            cp.start()
    total = part_ref[...]
    for k, cp in enumerate(first):
        cp.wait_recv()
        total = total + rbuf[k]
    rsum[...] = total
    second = [copy(rsum, cbuf.at[k], n_row - 1 + k, peer) for k, peer in enumerate(col_peers)]
    for cp in second:
        cp.start()
    for k, cp in enumerate(second):
        cp.wait_recv()
        total = total + cbuf[k]
    tot_ref[...] = total
    for cp in halos:
        cp.wait_recv()
    for cp in first + second + halos:
        cp.wait_send()


def exchange(part, n_row, n_col, x=None, edge=None):
    halo = x is not None
    out_shape = [jax.ShapeDtypeStruct((8, LANES), F32)]
    args = [part]
    in_specs = [VSPEC]
    if halo:
        n_img, n_rows, n_cols, n_chan = x.shape
        out_shape += [
            jax.ShapeDtypeStruct((n_img, n_cols, n_chan), BF16),
            jax.ShapeDtypeStruct((n_img, n_cols, n_chan), BF16),
            jax.ShapeDtypeStruct((2, n_rows + 2, n_img, n_chan), BF16),
        ]
        args += [x, edge]
        in_specs += [ASPEC, VSPEC]
    n_sem = n_row + n_col - 2 + (8 if halo else 0)
    return pl.pallas_call(
        functools.partial(exchange_kernel, n_row, n_col, halo),
        out_shape=out_shape,
        in_specs=in_specs,
        out_specs=[VSPEC] + [ASPEC] * (len(out_shape) - 1),
        scratch_shapes=[
            pltpu.VMEM((n_row - 1, 8, LANES), F32),
            pltpu.VMEM((n_col - 1, 8, LANES), F32),
            pltpu.VMEM((8, LANES), F32),
            pltpu.SemaphoreType.DMA((n_sem,)),
            pltpu.SemaphoreType.DMA((n_sem,)),
        ],
        compiler_params=pltpu.CompilerParams(collective_id=1 if halo else 2, has_side_effects=True, vmem_limit_bytes=VMEM_LIMIT),
        name="exchange",
    )(*args)


def conv_kernel(idx, n_row, n_col, count, residual, blk_ref, x_ref, top_ref, bot_ref, side_ref, tot_ref, norm_ref, add_ref, w_hbm,
                out_ref, edge_ref, part_ref, act, hside, stat, wbuf, acc, csum, sem):
    n_img, n_rows, n_cols, n_chan = x_ref.shape
    per_img = n_rows * n_cols
    blk = blk_ref[0]

    def fetch(dy):
        return pltpu.make_async_copy(w_hbm.at[blk, idx, dy], wbuf.at[dy], sem.at[dy])

    for dy in range(3):
        fetch(dy).start()
    r, c = lax.axis_index('row'), lax.axis_index('col')
    st = expand(channel_stats(tot_ref[...], count), n_chan)
    gain = norm_ref[blk, idx, 0:1, :].astype(F32)
    shift = norm_ref[blk, idx, 1:2, :].astype(F32)
    stat[0:2] = st[0:2]
    stat[2:4] = st[2:4] * gain
    stat[4:5] = shift

    for side in range(2):
        inside = (c > 0) if side == 0 else (c < n_col - 1)
        for i in range(n_rows + 2):
            ok = inside
            if i == 0:
                ok = ok & (r > 0)
            if i == n_rows + 1:
                ok = ok & (r < n_row - 1)
            z = side_ref[side, i].astype(F32)
            a = silu((z - stat[0:2]) * stat[2:4] + stat[4:5])
            hside[side, i] = jnp.where(ok, a, 0.0)

    step = 256

    def place(b, i, src, ok):
        rows = lax.broadcasted_iota(jnp.int32, (n_cols, step), 0)
        for ch in range(0, n_chan, step):
            sl = slice(ch, ch + step)
            z = src(sl).astype(F32)
            a = silu((z - stat[b:b + 1, sl]) * stat[2 + b:3 + b, sl] + stat[4:5, sl])
            if ok is not None:
                a = jnp.where(ok, a, 0.0)
            act[b, i, :, n_chan + ch:n_chan + ch + step] = a.astype(BF16)
            lo = jnp.where(rows == 0, hside[0, i, b:b + 1, sl], pltpu.roll(a, 1, 0))
            act[b, i, :, ch:ch + step] = lo.astype(BF16)
            hi = jnp.where(rows == n_cols - 1, hside[1, i, b:b + 1, sl], pltpu.roll(a, n_cols - 1, 0))
            act[b, i, :, 2 * n_chan + ch:2 * n_chan + ch + step] = hi.astype(BF16)

    for b in range(n_img):
        place(b, 0, lambda sl, b=b: top_ref[b, :, sl], r > 0)

        def middle(i, carry, b=b):
            place(b, i + 1, lambda sl: x_ref[b, i, :, sl], None)
            return carry

        lax.fori_loop(0, n_rows, middle, 0)
        place(b, n_rows + 1, lambda sl, b=b: bot_ref[b, :, sl], r < n_row - 1)

    if residual:
        acc[...] = add_ref[...].reshape(acc.shape).astype(F32)
    else:
        for b in range(n_img):
            acc[b * per_img:(b + 1) * per_img, :] = jnp.broadcast_to(add_ref[blk, b:b + 1, :], (per_img, n_chan))

    def taps(dy, carry):
        fetch(dy).wait()
        lhs = act[:, pl.ds(dy, n_rows)].reshape(n_img * per_img, 3 * n_chan)
        for ch in range(0, n_chan, 256):
            rhs = wbuf[dy, :, :, ch:ch + 256].reshape(3 * n_chan, 256)
            acc[:, ch:ch + 256] += jnp.dot(lhs, rhs, preferred_element_type=F32)
        return carry

    lax.fori_loop(0, 3, taps, 0)
    finish(acc, out_ref, edge_ref, part_ref, csum)


def conv(blk, idx, x, halos, norm, add, weights, n_row, n_col, residual):
    tot, top, bot, side = halos
    n_img, n_rows, n_cols, n_chan = x.shape
    count = float(n_rows * n_cols * n_row * n_col * (n_chan // GROUPS))
    n_tok = n_img * n_rows * n_cols
    return pl.pallas_call(
        functools.partial(conv_kernel, idx, n_row, n_col, count, residual),
        out_shape=[jax.ShapeDtypeStruct(x.shape, BF16)] + finish_shapes(x.shape),
        in_specs=[pl.BlockSpec(memory_space=pltpu.SMEM)] + [VSPEC] * 7 + [ASPEC],
        out_specs=[VSPEC] * 3,
        scratch_shapes=[
            pltpu.VMEM((n_img, n_rows + 2, n_cols, 3 * n_chan), BF16),
            pltpu.VMEM((2, n_rows + 2, n_img, n_chan), F32),
            pltpu.VMEM((8, n_chan), F32),
            pltpu.VMEM((3, 3, n_chan, n_chan), BF16),
            pltpu.VMEM((n_tok, n_chan), F32),
            pltpu.VMEM((8, n_chan), F32),
            pltpu.SemaphoreType.DMA((3,)),
        ],
        compiler_params=pltpu.CompilerParams(vmem_limit_bytes=VMEM_LIMIT),
        cost_estimate=pl.CostEstimate(flops=2 * 9 * n_tok * n_chan * n_chan, bytes_accessed=9 * 2 * n_chan * n_chan, transcendentals=n_tok * n_chan),
        name="conv",
    )(jnp.full((1,), blk, jnp.int32), x, top, bot, side, tot, norm, add, weights)


def head_blocks(per_dev):
    return [(i, min(2, per_dev - i)) for i in range(0, per_dev, 2)]


def send_plan(per_dev):
    blocks = head_blocks(per_dev)
    return [p for p in (blocks[:1], blocks[1:]) if p]


def proj_kernel(count, per_dev, x_ref, tot_ref, norm_ref, w_ref, *refs):
    n_img, n_rows, n_cols, n_chan = x_ref.shape
    per_img = n_rows * n_cols
    hd = w_ref.shape[2]
    plan = send_plan(per_dev)
    outs, g, wcat = refs[:len(plan)], refs[-2], refs[-1]

    @pl.when(pl.program_id(0) == 0)
    def _():
        st = expand(channel_stats(tot_ref[...], count), n_chan)
        gain = norm_ref[0:1, :].astype(F32)
        shift = norm_ref[1:2, :].astype(F32)
        for b in range(n_img):
            z = x_ref[b].reshape(per_img, n_chan).astype(F32)
            g[b * per_img:(b + 1) * per_img, :] = ((z - st[b:b + 1]) * (st[2 + b:3 + b] * gain) + shift).astype(BF16)

    for blocks, out_ref in zip(plan, outs):
        off = 0
        for first, n in blocks:
            for i in range(n):
                wcat[2 * i * hd:(2 * i + 1) * hd, :] = w_ref[1, first + i]
                wcat[(2 * i + 1) * hd:(2 * i + 2) * hd, :] = w_ref[2, first + i]
                wcat[(2 * n + i) * hd:(2 * n + i + 1) * hd, :] = w_ref[0, first + i]
            width = 2 * hd * (n + 1)
            if n == 1:
                wcat[3 * hd:width, :] = jnp.zeros((width - 3 * hd, n_chan), BF16)
            res = lax.dot_general(g[...], wcat[0:width, :], (((1,), (1,)), ((), ())), preferred_element_type=F32).astype(BF16)
            for b in range(n_img):
                out_ref[b, 0, :, off:off + width] = res[b * per_img:(b + 1) * per_img]
            off += width


def proj(x, tot, norm, weights, n_row, n_col, per_dev):
    n_img, n_rows, n_cols, n_chan = x.shape
    _, n_heads, hd, _ = weights.shape
    count = float(n_rows * n_cols * n_row * n_col * (n_chan // GROUPS))
    n_grp = n_heads // per_dev
    n_tok = n_rows * n_cols
    widths = [sum(2 * hd * (n + 1) for _, n in blocks) for blocks in send_plan(per_dev)]
    return pl.pallas_call(
        functools.partial(proj_kernel, count, per_dev),
        grid=(n_grp,),
        out_shape=[jax.ShapeDtypeStruct((n_img, n_grp, n_tok, w), BF16) for w in widths],
        in_specs=[
            pl.BlockSpec(x.shape, lambda q: (0, 0, 0, 0)),
            pl.BlockSpec((8, LANES), lambda q: (0, 0)),
            pl.BlockSpec(norm.shape, lambda q: (0, 0)),
            pl.BlockSpec((3, per_dev, hd, n_chan), lambda q: (0, q, 0, 0)),
        ],
        out_specs=[pl.BlockSpec((n_img, 1, n_tok, w), lambda q: (0, q, 0, 0)) for w in widths],
        scratch_shapes=[pltpu.VMEM((n_img * n_tok, n_chan), BF16), pltpu.VMEM((6 * hd, n_chan), BF16)],
        compiler_params=pltpu.CompilerParams(vmem_limit_bytes=VMEM_LIMIT),
        cost_estimate=pl.CostEstimate(flops=2 * n_img * n_tok * n_chan * n_grp * sum(widths), bytes_accessed=6 * n_chan * n_chan, transcendentals=0),
        name="proj",
    )(x, tot, norm, weights)


def attend_kernel(hd, n_pair, q_ref, kv_ref, out_ref, qt, qf, kk, vt, ot, w0, w1, osum, lsum, big):
    n_q, n_k = q_ref.shape[0], kv_ref.shape[0]
    half = pl.multiple_of(pl.program_id(0) * hd, hd)
    factor = 1.4426950408889634 * hd ** -0.5
    kb, qb = w0.shape
    tb = min(512, n_q)

    @pl.when(pl.program_id(0) == 0)
    def _():
        lane = lax.broadcasted_iota(jnp.int32, (n_k, 2 * hd), 1)
        kk[:, 2 * hd:] = jnp.where(lane == 0, 1.0, 0.0).astype(BF16)
        if n_pair == 1:
            ot[hd:, :] = jnp.zeros((hd, n_q), F32)

    def flip(t, top):
        at = pl.multiple_of(t * tb, tb)
        blk = kv_ref[pl.ds(at, tb), :].astype(F32)
        turned = blk.T
        vt[:, pl.ds(at, tb)] = turned[hd:].astype(BF16)
        lane = lax.broadcasted_iota(jnp.int32, blk.shape, 1)
        kk[pl.ds(at, tb), 0:2 * hd] = jnp.where(lane < hd, blk, pltpu.roll(blk, hd, 1)).astype(BF16)
        return jnp.maximum(top, jnp.sum(turned[:hd] * turned[:hd], axis=0, keepdims=True))

    top = lax.fori_loop(0, n_k // tb, flip, jnp.zeros((1, tb), F32))
    key_norm = jnp.sqrt(jnp.max(top, axis=1, keepdims=True))

    for t in range(0, n_q, tb):
        qf[:, t:t + tb] = q_ref[t:t + tb, :].astype(F32).T
    scaled = qf[pl.ds(half, hd), :] * factor
    high = scaled.astype(BF16)
    qt[0:hd, :] = high
    qt[hd:2 * hd, :] = (scaled - high.astype(F32)).astype(BF16)
    bound = jnp.sqrt(jnp.sum(scaled * scaled, axis=0, keepdims=True)) * key_norm
    row = lax.broadcasted_iota(jnp.int32, (2 * hd, n_q), 0)
    qt[2 * hd:, :] = jnp.where(row == 0, ROOM - bound, 0.0).astype(BF16)

    n_blk = n_k // kb

    def queries(t, carry):
        at = pl.multiple_of(t * qb, qb)
        rhs = qt[:, pl.ds(at, qb)]

        def weigh(s, dst):
            pos = pl.multiple_of(s * kb, kb)
            w = jnp.exp2(jnp.dot(kk[pl.ds(pos, kb), :], rhs, preferred_element_type=F32))
            dst[...] = w.astype(BF16)
            return jnp.sum(w.reshape(kb // 8, 8, qb), axis=0)

        def gather(s, src):
            pos = pl.multiple_of(s * kb, kb)
            osum[...] += jnp.dot(vt[:, pl.ds(pos, kb)], src[...], preferred_element_type=F32)

        osum[...] = jnp.zeros_like(osum)
        total = weigh(0, w0)

        def keys(j, total):
            total += weigh(2 * j + 1, w1)
            gather(2 * j, w0)
            total += weigh(2 * j + 2, w0)
            gather(2 * j + 1, w1)
            return total

        total = lax.fori_loop(0, n_blk // 2 - 1, keys, total)
        total += weigh(n_blk - 1, w1)
        gather(n_blk - 2, w0)
        gather(n_blk - 1, w1)
        total = jnp.sum(total, axis=0, keepdims=True)
        lsum[:, pl.ds(at, qb)] = total
        big[:, pl.ds(at, qb)] = jnp.max(jnp.abs(osum[...]), axis=0, keepdims=True)
        ot[pl.ds(half, hd), pl.ds(at, qb)] = osum[...] / total
        return carry

    lax.fori_loop(0, n_q // qb, queries, 0)
    sound = (jnp.min(lsum[...]) >= TINY) & (jnp.max(big[...]) <= 3e38) & (jnp.max(lsum[...]) <= 3e38)

    @pl.when(jnp.logical_not(sound))
    def _():
        qt[2 * hd:, :] = jnp.zeros((2 * hd, n_q), BF16)
        sk, sq = min(256, n_k), min(256, n_q)

        def some_queries(t, carry):
            at = pl.multiple_of(t * sq, sq)

            def some_keys(s, state):
                run_max, run_sum, out = state
                pos = pl.multiple_of(s * sk, sk)
                logits = jnp.dot(kk[pl.ds(pos, sk), :], qt[:, pl.ds(at, sq)], preferred_element_type=F32)
                new_max = jnp.maximum(run_max, jnp.max(logits, axis=0, keepdims=True))
                scale = jnp.exp2(run_max - new_max)
                w = jnp.exp2(logits - new_max)
                run_sum = run_sum * scale + jnp.sum(w, axis=0, keepdims=True)
                out = out * scale + jnp.dot(vt[:, pl.ds(pos, sk)], w.astype(BF16), preferred_element_type=F32)
                return new_max, run_sum, out

            init = (jnp.full((1, sq), -jnp.inf, F32), jnp.zeros((1, sq), F32), jnp.zeros((hd, sq), F32))
            _, run_sum, out = lax.fori_loop(0, n_k // sk, some_keys, init)
            ot[pl.ds(half, hd), pl.ds(at, sq)] = out / run_sum
            return carry

        lax.fori_loop(0, n_q // sq, some_queries, 0)

    for t in range(0, n_q, tb):
        out_ref[t:t + tb, :] = ot[:, t:t + tb].T.astype(BF16)


def attend(q, kv, hd, n_pair, kb=1024, qb=768):
    n_q, n_k = q.shape[0], kv.shape[0]
    kb, qb = min(kb, n_k // 2), min(qb, n_q)
    return pl.pallas_call(
        functools.partial(attend_kernel, hd, n_pair),
        grid=(n_pair,),
        out_shape=jax.ShapeDtypeStruct(q.shape, BF16),
        in_specs=[pl.BlockSpec((n_q, 2 * hd), lambda i: (0, 0)), pl.BlockSpec((n_k, 2 * hd), lambda i: (0, i))],
        out_specs=pl.BlockSpec((n_q, 2 * hd), lambda i: (0, 0)),
        scratch_shapes=[
            pltpu.VMEM((4 * hd, n_q), BF16),
            pltpu.VMEM((2 * hd, n_q), F32),
            pltpu.VMEM((n_k, 4 * hd), BF16),
            pltpu.VMEM((hd, n_k), BF16),
            pltpu.VMEM((2 * hd, n_q), F32),
            pltpu.VMEM((kb, qb), BF16),
            pltpu.VMEM((kb, qb), BF16),
            pltpu.VMEM((hd, qb), F32),
            pltpu.VMEM((1, n_q), F32),
            pltpu.VMEM((1, n_q), F32),
        ],
        compiler_params=pltpu.CompilerParams(vmem_limit_bytes=VMEM_LIMIT),
        cost_estimate=pl.CostEstimate(flops=16 * n_pair * n_q * n_k * hd, bytes_accessed=n_pair * n_k * hd * 4, transcendentals=n_pair * n_q * n_k),
        name="attend",
    )(q, kv)


def outproj_kernel(n_in, *refs):
    o_refs = refs[:n_in]
    w_ref, x_ref, out_ref, edge_ref, part_ref, wcat, acc, csum = refs[n_in:]
    n_img, n_rows, n_cols, n_chan = x_ref.shape
    per_dev, hd, _ = w_ref.shape[1:]
    per_img = n_rows * n_cols
    q = pl.program_id(0)

    @pl.when(q == 0)
    def _():
        acc[...] = x_ref[...].reshape(acc.shape).astype(F32)
        wcat[per_dev * hd:, :] = jnp.zeros((wcat.shape[0] - per_dev * hd, n_chan), BF16)

    for i in range(per_dev):
        wcat[i * hd:(i + 1) * hd, :] = w_ref[0, i]
    lhs = jnp.concatenate([o[:, 0].reshape(n_img * per_img, o.shape[3]) for o in o_refs], axis=1)
    for n in range(0, n_chan, 256):
        acc[:, n:n + 256] += jnp.dot(lhs, wcat[:, n:n + 256], preferred_element_type=F32)

    @pl.when(q == pl.num_programs(0) - 1)
    def _():
        finish(acc, out_ref, edge_ref, part_ref, csum)


def outproj(outs, weights, x, per_dev):
    n_img, n_grp, n_tok, width = outs[0].shape
    _, n_heads, hd, n_chan = weights.shape
    shapes = [jax.ShapeDtypeStruct(x.shape, BF16)] + finish_shapes(x.shape)
    return pl.pallas_call(
        functools.partial(outproj_kernel, len(outs)),
        grid=(n_grp,),
        out_shape=shapes,
        in_specs=[pl.BlockSpec((n_img, 1, n_tok, width), lambda q: (0, q, 0, 0)) for _ in outs] + [
            pl.BlockSpec((1, per_dev, hd, n_chan), lambda q: (3, q, 0, 0)),
            pl.BlockSpec(x.shape, lambda q: (0, 0, 0, 0)),
        ],
        out_specs=[pl.BlockSpec(s.shape, lambda q, n=len(s.shape): (0,) * n) for s in shapes],
        scratch_shapes=[pltpu.VMEM((len(outs) * width, n_chan), BF16), pltpu.VMEM((n_img * n_tok, n_chan), F32), pltpu.VMEM((8, n_chan), F32)],
        compiler_params=pltpu.CompilerParams(vmem_limit_bytes=VMEM_LIMIT),
        cost_estimate=pl.CostEstimate(flops=2 * n_img * n_tok * n_chan * n_chan, bytes_accessed=2 * n_chan * n_chan, transcendentals=0),
        name="outproj",
    )(*outs, weights, x)


def solution(mesh):
    n_row, n_col = mesh.shape['row'], mesh.shape['col']

    def res_block(blk, x, edge, part, t_proj, res_norm, res_conv):
        halos = exchange(part, n_row, n_col, x, edge)
        h, edge, part = conv(blk, 0, x, halos, res_norm, t_proj, res_conv, n_row, n_col, False)
        halos = exchange(part, n_row, n_col, h, edge)
        return conv(blk, 1, h, halos, res_norm, x, res_conv, n_row, n_col, True)

    def attn_block(x, part, norm, weights):
        n_img, n_rows, n_cols, n_chan = x.shape
        weights = jnp.swapaxes(weights, 2, 3)
        n_heads, hd = weights.shape[1], weights.shape[2]
        per_dev = n_img * n_heads // n_row
        n_tok = n_rows * n_cols
        tot, = exchange(part, n_row, n_col)
        qkv = proj(x, tot, norm, weights, n_row, n_col, per_dev)
        outs = []
        for sent, blocks in zip(qkv, send_plan(per_dev)):
            mine = lax.all_to_all(sent.reshape(n_row, n_tok, -1), 'row', 0, 0).reshape(n_row * n_tok, -1)
            off = 0
            for _, n_pair in blocks:
                mid, end = off + n_pair * 2 * hd, off + (n_pair + 1) * 2 * hd
                kv = lax.all_gather(mine[:, off:mid], 'col', axis=0, tiled=True)
                out = attend(mine[:, mid:end], kv, hd, n_pair)
                out = lax.all_to_all(out.reshape(n_row, n_tok, 2 * hd), 'row', 0, 0)
                outs.append(out.reshape(n_img, -1, n_tok, 2 * hd))
                off = end
        return outproj(outs, weights, x, per_dev)

    def run_stage(latent, t_emb, res_norm, res_conv, res_temb, attn_norm, attn_proj):
        edge, part, t_proj = prep(latent, t_emb, res_temb)
        x, edge, part = res_block(0, latent, edge, part, t_proj, res_norm, res_conv)
        x, edge, part = attn_block(x, part, attn_norm, attn_proj)
        return res_block(1, x, edge, part, t_proj, res_norm, res_conv)[0]

    spec_x = P('dp', 'row', 'col', None)
    return jax.shard_map(run_stage, mesh=mesh, in_specs=(spec_x, P('dp', None), P(), P(), P(), P(), P()), out_specs=spec_x, check_vma=False)
```

```python
import functools

import jax
import jax.numpy as jnp
from jax import lax
from jax.experimental import pallas as pl
from jax.experimental.pallas import tpu as pltpu
from jax.sharding import PartitionSpec as P

GROUPS = 32
EPS = 1e-5
LANES = 128
ROOM = 60.0
TINY = 2.0 ** -90
MESH = pl.DeviceIdType.MESH
HIGH = lax.Precision.HIGHEST
F32 = jnp.float32
BF16 = jnp.bfloat16
VMEM_LIMIT = 60 * 1024 * 1024
VSPEC = pl.BlockSpec(memory_space=pltpu.VMEM)
ASPEC = pl.BlockSpec(memory_space=pl.ANY)


def group_mask(n_chan, chan_axis):
    width = n_chan // GROUPS
    shape = (n_chan, LANES) if chan_axis == 0 else (LANES, n_chan)
    chan = lax.broadcasted_iota(jnp.int32, shape, chan_axis)
    first = lax.broadcasted_iota(jnp.int32, shape, 1 - chan_axis) * width
    return jnp.where((chan >= first) & (chan < first + width), 1.0, 0.0).astype(F32)


def channel_stats(tot, count):
    vals = tot / count
    mean = vals[0:2]
    inv = lax.rsqrt(vals[2:4] - mean * mean + EPS)
    return jnp.concatenate([mean, inv, jnp.zeros((4, LANES), F32)], axis=0)


def expand(stats, n_chan):
    return jnp.dot(stats, group_mask(n_chan, 1), precision=HIGH, preferred_element_type=F32)


def silu(u):
    half = 0.5 * u
    return half * jnp.tanh(half) + half


def finish(acc, out_ref, edge_ref, part_ref, csum):
    n_img, n_rows, n_cols, n_chan = out_ref.shape
    per_img = n_rows * n_cols
    csum[...] = jnp.zeros_like(csum)
    for ch in range(0, n_chan, 256):
        sl = slice(ch, ch + 256)
        for b in range(n_img):
            val = acc[b * per_img:(b + 1) * per_img, sl].astype(BF16)
            out_ref[b, :, :, sl] = val.reshape(n_rows, n_cols, 256)
            val = val.astype(F32)
            csum[b:b + 1, sl] = jnp.sum(val, axis=0, keepdims=True)
            csum[2 + b:3 + b, sl] = jnp.sum(val * val, axis=0, keepdims=True)
    for side, col in ((0, 0), (1, n_cols - 1)):
        for i in range(n_rows):
            rows = [acc[b * per_img + i * n_cols + col:b * per_img + i * n_cols + col + 1, :] for b in range(n_img)]
            edge_ref[side, i] = jnp.concatenate(rows, axis=0).astype(BF16)
    part_ref[...] = jnp.dot(csum[...], group_mask(n_chan, 0), precision=HIGH, preferred_element_type=F32)


def prep_kernel(x_ref, emb_ref, w_hbm, edge_ref, part_ref, t_ref, acc, dump, csum, wbuf, sem):
    n_blk = w_hbm.shape[0]
    loads = [pltpu.make_async_copy(w_hbm.at[k], wbuf.at[k], sem.at[k]) for k in range(n_blk)]
    for cp in loads:
        cp.start()
    acc[...] = x_ref[...].reshape(acc.shape).astype(F32)
    finish(acc, dump, edge_ref, part_ref, csum)
    emb = silu(emb_ref[...].astype(F32))
    n_img = emb.shape[0]
    emb = jnp.concatenate([emb, jnp.zeros((8 - n_img, emb.shape[1]), F32)], axis=0).astype(BF16)
    for k, cp in enumerate(loads):
        cp.wait()
        t_ref[k] = jnp.dot(emb, wbuf[k], preferred_element_type=F32)[0:n_img]


def finish_shapes(shape):
    n_img, n_rows, n_cols, n_chan = shape
    return [jax.ShapeDtypeStruct((2, n_rows, n_img, n_chan), BF16), jax.ShapeDtypeStruct((8, LANES), F32)]


def prep(x, t_emb, w_temb):
    n_img, n_rows, n_cols, n_chan = x.shape
    return pl.pallas_call(
        prep_kernel,
        out_shape=finish_shapes(x.shape) + [jax.ShapeDtypeStruct((w_temb.shape[0], n_img, n_chan), F32)],
        in_specs=[VSPEC, VSPEC, ASPEC],
        out_specs=[VSPEC, VSPEC, VSPEC],
        scratch_shapes=[
            pltpu.VMEM((n_img * n_rows * n_cols, n_chan), F32),
            pltpu.VMEM(x.shape, BF16),
            pltpu.VMEM((8, n_chan), F32),
            pltpu.VMEM(w_temb.shape, BF16),
            pltpu.SemaphoreType.DMA((w_temb.shape[0],)),
        ],
        compiler_params=pltpu.CompilerParams(vmem_limit_bytes=VMEM_LIMIT),
        name="prep",
    )(x, t_emb, w_temb)


def exchange_kernel(n_row, n_col, halo, *refs):
    if halo:
        part_ref, x_ref, edge_ref, tot_ref, top_ref, bot_ref, side_ref, rbuf, cbuf, rsum, send, recv = refs
    else:
        part_ref, tot_ref, rbuf, cbuf, rsum, send, recv = refs
    r, c = lax.axis_index('row'), lax.axis_index('col')
    up, down = lax.rem(r + n_row - 1, n_row), lax.rem(r + 1, n_row)
    left, right = lax.rem(c + n_col - 1, n_col), lax.rem(c + 1, n_col)
    row_peers = [{'row': lax.rem(r + k, n_row)} for k in range(1, n_row)]
    col_peers = [{'col': lax.rem(c + k, n_col)} for k in range(1, n_col)]
    diag = [{'row': a, 'col': b} for a in (up, down) for b in (left, right)] if halo else []
    peers = row_peers + col_peers + diag
    barrier = pltpu.get_barrier_semaphore()
    for peer in peers:
        pl.semaphore_signal(barrier, inc=1, device_id=peer, device_id_type=MESH)
    pl.semaphore_wait(barrier, len(peers))

    def copy(src, dst, slot, peer):
        return pltpu.make_async_remote_copy(src_ref=src, dst_ref=dst, send_sem=send.at[slot], recv_sem=recv.at[slot], device_id=peer, device_id_type=MESH)

    first = [copy(part_ref, rbuf.at[k], k, peer) for k, peer in enumerate(row_peers)]
    for cp in first:
        cp.start()
    halos = []
    if halo:
        last = x_ref.shape[1] - 1
        end = side_ref.shape[1] - 1
        plan = [
            (x_ref.at[:, last], top_ref, {'row': down}),
            (x_ref.at[:, 0], bot_ref, {'row': up}),
            (edge_ref.at[0], side_ref.at[1, 1:end], {'col': left}),
            (edge_ref.at[1], side_ref.at[0, 1:end], {'col': right}),
            (edge_ref.at[0, 0], side_ref.at[1, end], {'row': up, 'col': left}),
            (edge_ref.at[0, last], side_ref.at[1, 0], {'row': down, 'col': left}),
            (edge_ref.at[1, 0], side_ref.at[0, end], {'row': up, 'col': right}),
            (edge_ref.at[1, last], side_ref.at[0, 0], {'row': down, 'col': right}),
        ]
        halos = [copy(src, dst, n_row + n_col - 2 + i, peer) for i, (src, dst, peer) in enumerate(plan)]
        for cp in halos:
            cp.start()
    total = part_ref[...]
    for k, cp in enumerate(first):
        cp.wait_recv()
        total = total + rbuf[k]
    rsum[...] = total
    second = [copy(rsum, cbuf.at[k], n_row - 1 + k, peer) for k, peer in enumerate(col_peers)]
    for cp in second:
        cp.start()
    for k, cp in enumerate(second):
        cp.wait_recv()
        total = total + cbuf[k]
    tot_ref[...] = total
    for cp in halos:
        cp.wait_recv()
    for cp in first + second + halos:
        cp.wait_send()


def exchange(part, n_row, n_col, x=None, edge=None):
    halo = x is not None
    out_shape = [jax.ShapeDtypeStruct((8, LANES), F32)]
    args = [part]
    in_specs = [VSPEC]
    if halo:
        n_img, n_rows, n_cols, n_chan = x.shape
        out_shape += [
            jax.ShapeDtypeStruct((n_img, n_cols, n_chan), BF16),
            jax.ShapeDtypeStruct((n_img, n_cols, n_chan), BF16),
            jax.ShapeDtypeStruct((2, n_rows + 2, n_img, n_chan), BF16),
        ]
        args += [x, edge]
        in_specs += [ASPEC, VSPEC]
    n_sem = n_row + n_col - 2 + (8 if halo else 0)
    return pl.pallas_call(
        functools.partial(exchange_kernel, n_row, n_col, halo),
        out_shape=out_shape,
        in_specs=in_specs,
        out_specs=[VSPEC] + [ASPEC] * (len(out_shape) - 1),
        scratch_shapes=[
            pltpu.VMEM((n_row - 1, 8, LANES), F32),
            pltpu.VMEM((n_col - 1, 8, LANES), F32),
            pltpu.VMEM((8, LANES), F32),
            pltpu.SemaphoreType.DMA((n_sem,)),
            pltpu.SemaphoreType.DMA((n_sem,)),
        ],
        compiler_params=pltpu.CompilerParams(collective_id=1 if halo else 2, has_side_effects=True, vmem_limit_bytes=VMEM_LIMIT),
        name="exchange",
    )(*args)


def conv_kernel(blk, idx, n_row, n_col, count, residual, x_ref, top_ref, bot_ref, side_ref, tot_ref, norm_ref, add_ref, w_hbm,
                out_ref, edge_ref, part_ref, act, hside, stat, wbuf, acc, csum, sem):
    n_img, n_rows, n_cols, n_chan = x_ref.shape
    per_img = n_rows * n_cols

    def fetch(dy):
        return pltpu.make_async_copy(w_hbm.at[blk, idx, dy], wbuf.at[dy], sem.at[dy])

    for dy in range(3):
        fetch(dy).start()
    r, c = lax.axis_index('row'), lax.axis_index('col')
    st = expand(channel_stats(tot_ref[...], count), n_chan)
    gain = norm_ref[blk, idx, 0:1, :].astype(F32)
    shift = norm_ref[blk, idx, 1:2, :].astype(F32)
    stat[0:2] = st[0:2]
    stat[2:4] = st[2:4] * gain
    stat[4:5] = shift

    for side in range(2):
        inside = (c > 0) if side == 0 else (c < n_col - 1)
        for i in range(n_rows + 2):
            ok = inside
            if i == 0:
                ok = ok & (r > 0)
            if i == n_rows + 1:
                ok = ok & (r < n_row - 1)
            z = side_ref[side, i].astype(F32)
            a = silu((z - stat[0:2]) * stat[2:4] + stat[4:5])
            hside[side, i] = jnp.where(ok, a, 0.0)

    step = 256

    def place(b, i, src, ok):
        rows = lax.broadcasted_iota(jnp.int32, (n_cols, step), 0)
        for ch in range(0, n_chan, step):
            sl = slice(ch, ch + step)
            z = src(sl).astype(F32)
            a = silu((z - stat[b:b + 1, sl]) * stat[2 + b:3 + b, sl] + stat[4:5, sl])
            if ok is not None:
                a = jnp.where(ok, a, 0.0)
            act[b, i, :, n_chan + ch:n_chan + ch + step] = a.astype(BF16)
            lo = jnp.where(rows == 0, hside[0, i, b:b + 1, sl], pltpu.roll(a, 1, 0))
            act[b, i, :, ch:ch + step] = lo.astype(BF16)
            hi = jnp.where(rows == n_cols - 1, hside[1, i, b:b + 1, sl], pltpu.roll(a, n_cols - 1, 0))
            act[b, i, :, 2 * n_chan + ch:2 * n_chan + ch + step] = hi.astype(BF16)

    for b in range(n_img):
        place(b, 0, lambda sl, b=b: top_ref[b, :, sl], r > 0)

        def middle(i, carry, b=b):
            place(b, i + 1, lambda sl: x_ref[b, i, :, sl], None)
            return carry

        lax.fori_loop(0, n_rows, middle, 0)
        place(b, n_rows + 1, lambda sl, b=b: bot_ref[b, :, sl], r < n_row - 1)

    if residual:
        acc[...] = add_ref[...].reshape(acc.shape).astype(F32)
    else:
        for b in range(n_img):
            acc[b * per_img:(b + 1) * per_img, :] = jnp.broadcast_to(add_ref[blk, b:b + 1, :], (per_img, n_chan))

    def taps(dy, carry):
        fetch(dy).wait()
        lhs = act[:, pl.ds(dy, n_rows)].reshape(n_img * per_img, 3 * n_chan)
        for ch in range(0, n_chan, 256):
            rhs = wbuf[dy, :, :, ch:ch + 256].reshape(3 * n_chan, 256)
            acc[:, ch:ch + 256] += jnp.dot(lhs, rhs, preferred_element_type=F32)
        return carry

    lax.fori_loop(0, 3, taps, 0)
    finish(acc, out_ref, edge_ref, part_ref, csum)


def conv(blk, idx, x, halos, norm, add, weights, n_row, n_col, residual):
    tot, top, bot, side = halos
    n_img, n_rows, n_cols, n_chan = x.shape
    count = float(n_rows * n_cols * n_row * n_col * (n_chan // GROUPS))
    n_tok = n_img * n_rows * n_cols
    return pl.pallas_call(
        functools.partial(conv_kernel, blk, idx, n_row, n_col, count, residual),
        out_shape=[jax.ShapeDtypeStruct(x.shape, BF16)] + finish_shapes(x.shape),
        in_specs=[VSPEC] * 7 + [ASPEC],
        out_specs=[VSPEC] * 3,
        scratch_shapes=[
            pltpu.VMEM((n_img, n_rows + 2, n_cols, 3 * n_chan), BF16),
            pltpu.VMEM((2, n_rows + 2, n_img, n_chan), F32),
            pltpu.VMEM((8, n_chan), F32),
            pltpu.VMEM((3, 3, n_chan, n_chan), BF16),
            pltpu.VMEM((n_tok, n_chan), F32),
            pltpu.VMEM((8, n_chan), F32),
            pltpu.SemaphoreType.DMA((3,)),
        ],
        compiler_params=pltpu.CompilerParams(vmem_limit_bytes=VMEM_LIMIT),
        cost_estimate=pl.CostEstimate(flops=2 * 9 * n_tok * n_chan * n_chan, bytes_accessed=9 * 2 * n_chan * n_chan, transcendentals=n_tok * n_chan),
        name="conv",
    )(x, top, bot, side, tot, norm, add, weights)


def head_blocks(per_dev):
    return [(i, min(2, per_dev - i)) for i in range(0, per_dev, 2)]


def send_plan(per_dev):
    blocks = head_blocks(per_dev)
    return [p for p in (blocks[:1], blocks[1:]) if p]


def proj_kernel(count, per_dev, x_ref, tot_ref, norm_ref, w_ref, *refs):
    n_img, n_rows, n_cols, n_chan = x_ref.shape
    per_img = n_rows * n_cols
    hd = w_ref.shape[2]
    plan = send_plan(per_dev)
    outs, g, wcat = refs[:len(plan)], refs[-2], refs[-1]

    @pl.when(pl.program_id(0) == 0)
    def _():
        st = expand(channel_stats(tot_ref[...], count), n_chan)
        gain = norm_ref[0:1, :].astype(F32)
        shift = norm_ref[1:2, :].astype(F32)
        for b in range(n_img):
            z = x_ref[b].reshape(per_img, n_chan).astype(F32)
            g[b * per_img:(b + 1) * per_img, :] = ((z - st[b:b + 1]) * (st[2 + b:3 + b] * gain) + shift).astype(BF16)

    for blocks, out_ref in zip(plan, outs):
        off = 0
        for first, n in blocks:
            for i in range(n):
                wcat[2 * i * hd:(2 * i + 1) * hd, :] = w_ref[1, first + i]
                wcat[(2 * i + 1) * hd:(2 * i + 2) * hd, :] = w_ref[2, first + i]
                wcat[(2 * n + i) * hd:(2 * n + i + 1) * hd, :] = w_ref[0, first + i]
            width = 2 * hd * (n + 1)
            if n == 1:
                wcat[3 * hd:width, :] = jnp.zeros((width - 3 * hd, n_chan), BF16)
            res = lax.dot_general(g[...], wcat[0:width, :], (((1,), (1,)), ((), ())), preferred_element_type=F32).astype(BF16)
            for b in range(n_img):
                out_ref[b, 0, :, off:off + width] = res[b * per_img:(b + 1) * per_img]
            off += width


def proj(x, tot, norm, weights, n_row, n_col, per_dev):
    n_img, n_rows, n_cols, n_chan = x.shape
    _, n_heads, hd, _ = weights.shape
    count = float(n_rows * n_cols * n_row * n_col * (n_chan // GROUPS))
    n_grp = n_heads // per_dev
    n_tok = n_rows * n_cols
    widths = [sum(2 * hd * (n + 1) for _, n in blocks) for blocks in send_plan(per_dev)]
    return pl.pallas_call(
        functools.partial(proj_kernel, count, per_dev),
        grid=(n_grp,),
        out_shape=[jax.ShapeDtypeStruct((n_img, n_grp, n_tok, w), BF16) for w in widths],
        in_specs=[
            pl.BlockSpec(x.shape, lambda q: (0, 0, 0, 0)),
            pl.BlockSpec((8, LANES), lambda q: (0, 0)),
            pl.BlockSpec(norm.shape, lambda q: (0, 0)),
            pl.BlockSpec((3, per_dev, hd, n_chan), lambda q: (0, q, 0, 0)),
        ],
        out_specs=[pl.BlockSpec((n_img, 1, n_tok, w), lambda q: (0, q, 0, 0)) for w in widths],
        scratch_shapes=[pltpu.VMEM((n_img * n_tok, n_chan), BF16), pltpu.VMEM((6 * hd, n_chan), BF16)],
        compiler_params=pltpu.CompilerParams(vmem_limit_bytes=VMEM_LIMIT),
        cost_estimate=pl.CostEstimate(flops=2 * n_img * n_tok * n_chan * n_grp * sum(widths), bytes_accessed=6 * n_chan * n_chan, transcendentals=0),
        name="proj",
    )(x, tot, norm, weights)


def attend_kernel(hd, n_pair, q_ref, kv_ref, out_ref, qt, qf, kk, vt, ot, w0, w1, osum, lsum, big):
    n_q, n_k = q_ref.shape[0], kv_ref.shape[0]
    half = pl.multiple_of(pl.program_id(0) * hd, hd)
    factor = 1.4426950408889634 * hd ** -0.5
    kb, qb = w0.shape
    tb = min(512, n_q)

    @pl.when(pl.program_id(0) == 0)
    def _():
        lane = lax.broadcasted_iota(jnp.int32, (n_k, 2 * hd), 1)
        kk[:, 2 * hd:] = jnp.where(lane == 0, 1.0, 0.0).astype(BF16)
        if n_pair == 1:
            ot[hd:, :] = jnp.zeros((hd, n_q), F32)

    def flip(t, top):
        at = pl.multiple_of(t * tb, tb)
        blk = kv_ref[pl.ds(at, tb), :].astype(F32)
        turned = blk.T
        vt[:, pl.ds(at, tb)] = turned[hd:].astype(BF16)
        lane = lax.broadcasted_iota(jnp.int32, blk.shape, 1)
        kk[pl.ds(at, tb), 0:2 * hd] = jnp.where(lane < hd, blk, pltpu.roll(blk, hd, 1)).astype(BF16)
        return jnp.maximum(top, jnp.sum(turned[:hd] * turned[:hd], axis=0, keepdims=True))

    top = lax.fori_loop(0, n_k // tb, flip, jnp.zeros((1, tb), F32))
    key_norm = jnp.sqrt(jnp.max(top, axis=1, keepdims=True))

    for t in range(0, n_q, tb):
        qf[:, t:t + tb] = q_ref[t:t + tb, :].astype(F32).T
    scaled = qf[pl.ds(half, hd), :] * factor
    high = scaled.astype(BF16)
    qt[0:hd, :] = high
    qt[hd:2 * hd, :] = (scaled - high.astype(F32)).astype(BF16)
    bound = jnp.sqrt(jnp.sum(scaled * scaled, axis=0, keepdims=True)) * key_norm
    row = lax.broadcasted_iota(jnp.int32, (2 * hd, n_q), 0)
    qt[2 * hd:, :] = jnp.where(row == 0, ROOM - bound, 0.0).astype(BF16)

    n_blk = n_k // kb

    def queries(t, carry):
        at = pl.multiple_of(t * qb, qb)
        rhs = qt[:, pl.ds(at, qb)]

        def weigh(s, dst):
            pos = pl.multiple_of(s * kb, kb)
            w = jnp.exp2(jnp.dot(kk[pl.ds(pos, kb), :], rhs, preferred_element_type=F32))
            dst[...] = w.astype(BF16)
            return jnp.sum(w.reshape(kb // 8, 8, qb), axis=0)

        def gather(s, src):
            pos = pl.multiple_of(s * kb, kb)
            osum[...] += jnp.dot(vt[:, pl.ds(pos, kb)], src[...], preferred_element_type=F32)

        osum[...] = jnp.zeros_like(osum)
        total = weigh(0, w0)

        def keys(j, total):
            total += weigh(2 * j + 1, w1)
            gather(2 * j, w0)
            total += weigh(2 * j + 2, w0)
            gather(2 * j + 1, w1)
            return total

        total = lax.fori_loop(0, n_blk // 2 - 1, keys, total)
        total += weigh(n_blk - 1, w1)
        gather(n_blk - 2, w0)
        gather(n_blk - 1, w1)
        total = jnp.sum(total, axis=0, keepdims=True)
        lsum[:, pl.ds(at, qb)] = total
        big[:, pl.ds(at, qb)] = jnp.max(jnp.abs(osum[...]), axis=0, keepdims=True)
        ot[pl.ds(half, hd), pl.ds(at, qb)] = osum[...] / total
        return carry

    lax.fori_loop(0, n_q // qb, queries, 0)
    sound = (jnp.min(lsum[...]) >= TINY) & (jnp.max(big[...]) <= 3e38) & (jnp.max(lsum[...]) <= 3e38)

    @pl.when(jnp.logical_not(sound))
    def _():
        qt[2 * hd:, :] = jnp.zeros((2 * hd, n_q), BF16)
        sk, sq = min(256, n_k), min(256, n_q)

        def some_queries(t, carry):
            at = pl.multiple_of(t * sq, sq)

            def some_keys(s, state):
                run_max, run_sum, out = state
                pos = pl.multiple_of(s * sk, sk)
                logits = jnp.dot(kk[pl.ds(pos, sk), :], qt[:, pl.ds(at, sq)], preferred_element_type=F32)
                new_max = jnp.maximum(run_max, jnp.max(logits, axis=0, keepdims=True))
                scale = jnp.exp2(run_max - new_max)
                w = jnp.exp2(logits - new_max)
                run_sum = run_sum * scale + jnp.sum(w, axis=0, keepdims=True)
                out = out * scale + jnp.dot(vt[:, pl.ds(pos, sk)], w.astype(BF16), preferred_element_type=F32)
                return new_max, run_sum, out

            init = (jnp.full((1, sq), -jnp.inf, F32), jnp.zeros((1, sq), F32), jnp.zeros((hd, sq), F32))
            _, run_sum, out = lax.fori_loop(0, n_k // sk, some_keys, init)
            ot[pl.ds(half, hd), pl.ds(at, sq)] = out / run_sum
            return carry

        lax.fori_loop(0, n_q // sq, some_queries, 0)

    for t in range(0, n_q, tb):
        out_ref[t:t + tb, :] = ot[:, t:t + tb].T.astype(BF16)


def attend(q, kv, hd, n_pair, kb=1024, qb=768):
    n_q, n_k = q.shape[0], kv.shape[0]
    kb, qb = min(kb, n_k // 2), min(qb, n_q)
    return pl.pallas_call(
        functools.partial(attend_kernel, hd, n_pair),
        grid=(n_pair,),
        out_shape=jax.ShapeDtypeStruct(q.shape, BF16),
        in_specs=[pl.BlockSpec((n_q, 2 * hd), lambda i: (0, 0)), pl.BlockSpec((n_k, 2 * hd), lambda i: (0, i))],
        out_specs=pl.BlockSpec((n_q, 2 * hd), lambda i: (0, 0)),
        scratch_shapes=[
            pltpu.VMEM((4 * hd, n_q), BF16),
            pltpu.VMEM((2 * hd, n_q), F32),
            pltpu.VMEM((n_k, 4 * hd), BF16),
            pltpu.VMEM((hd, n_k), BF16),
            pltpu.VMEM((2 * hd, n_q), F32),
            pltpu.VMEM((kb, qb), BF16),
            pltpu.VMEM((kb, qb), BF16),
            pltpu.VMEM((hd, qb), F32),
            pltpu.VMEM((1, n_q), F32),
            pltpu.VMEM((1, n_q), F32),
        ],
        compiler_params=pltpu.CompilerParams(vmem_limit_bytes=VMEM_LIMIT),
        cost_estimate=pl.CostEstimate(flops=16 * n_pair * n_q * n_k * hd, bytes_accessed=n_pair * n_k * hd * 4, transcendentals=n_pair * n_q * n_k),
        name="attend",
    )(q, kv)


def outproj_kernel(n_in, *refs):
    o_refs = refs[:n_in]
    w_ref, x_ref, out_ref, edge_ref, part_ref, wcat, acc, csum = refs[n_in:]
    n_img, n_rows, n_cols, n_chan = x_ref.shape
    per_dev, hd, _ = w_ref.shape[1:]
    per_img = n_rows * n_cols
    q = pl.program_id(0)

    @pl.when(q == 0)
    def _():
        acc[...] = x_ref[...].reshape(acc.shape).astype(F32)
        wcat[per_dev * hd:, :] = jnp.zeros((wcat.shape[0] - per_dev * hd, n_chan), BF16)

    for i in range(per_dev):
        wcat[i * hd:(i + 1) * hd, :] = w_ref[0, i]
    lhs = jnp.concatenate([o[:, 0].reshape(n_img * per_img, o.shape[3]) for o in o_refs], axis=1)
    for n in range(0, n_chan, 256):
        acc[:, n:n + 256] += jnp.dot(lhs, wcat[:, n:n + 256], preferred_element_type=F32)

    @pl.when(q == pl.num_programs(0) - 1)
    def _():
        finish(acc, out_ref, edge_ref, part_ref, csum)


def outproj(outs, weights, x, per_dev):
    n_img, n_grp, n_tok, width = outs[0].shape
    _, n_heads, hd, n_chan = weights.shape
    shapes = [jax.ShapeDtypeStruct(x.shape, BF16)] + finish_shapes(x.shape)
    return pl.pallas_call(
        functools.partial(outproj_kernel, len(outs)),
        grid=(n_grp,),
        out_shape=shapes,
        in_specs=[pl.BlockSpec((n_img, 1, n_tok, width), lambda q: (0, q, 0, 0)) for _ in outs] + [
            pl.BlockSpec((1, per_dev, hd, n_chan), lambda q: (3, q, 0, 0)),
            pl.BlockSpec(x.shape, lambda q: (0, 0, 0, 0)),
        ],
        out_specs=[pl.BlockSpec(s.shape, lambda q, n=len(s.shape): (0,) * n) for s in shapes],
        scratch_shapes=[pltpu.VMEM((len(outs) * width, n_chan), BF16), pltpu.VMEM((n_img * n_tok, n_chan), F32), pltpu.VMEM((8, n_chan), F32)],
        compiler_params=pltpu.CompilerParams(vmem_limit_bytes=VMEM_LIMIT),
        cost_estimate=pl.CostEstimate(flops=2 * n_img * n_tok * n_chan * n_chan, bytes_accessed=2 * n_chan * n_chan, transcendentals=0),
        name="outproj",
    )(*outs, weights, x)


def solution(mesh):
    n_row, n_col = mesh.shape['row'], mesh.shape['col']

    def res_block(blk, x, edge, part, t_proj, res_norm, res_conv):
        halos = exchange(part, n_row, n_col, x, edge)
        h, edge, part = conv(blk, 0, x, halos, res_norm, t_proj, res_conv, n_row, n_col, False)
        halos = exchange(part, n_row, n_col, h, edge)
        return conv(blk, 1, h, halos, res_norm, x, res_conv, n_row, n_col, True)

    def attn_block(x, part, norm, weights):
        n_img, n_rows, n_cols, n_chan = x.shape
        weights = jnp.swapaxes(weights, 2, 3)
        n_heads, hd = weights.shape[1], weights.shape[2]
        per_dev = n_img * n_heads // n_row
        n_tok = n_rows * n_cols
        tot, = exchange(part, n_row, n_col)
        qkv = proj(x, tot, norm, weights, n_row, n_col, per_dev)
        parts = []
        mine = None
        for sent, blocks in zip(qkv, send_plan(per_dev)):
            if mine is not None:
                sent, mine = lax.optimization_barrier((sent, mine))
            mine = lax.all_to_all(sent.reshape(n_row, n_tok, -1), 'row', 0, 0).reshape(n_row * n_tok, -1)
            off = 0
            for _, n_pair in blocks:
                mid, end = off + n_pair * 2 * hd, off + (n_pair + 1) * 2 * hd
                parts.append([mine[:, mid:end], mine[:, off:mid], n_pair])
                off = end
        outs = []
        out = None
        for k, (q, kv, n_pair) in enumerate(parts):
            full = lax.all_gather(kv, 'col', axis=0, tiled=True)
            if k + 1 < len(parts):
                if out is not None:
                    parts[k + 1][1], out = lax.optimization_barrier((parts[k + 1][1], out))
                q, parts[k + 1][1] = lax.optimization_barrier((q, parts[k + 1][1]))
            out = attend(q, full, hd, n_pair)
            back = lax.all_to_all(out.reshape(n_row, n_tok, 2 * hd), 'row', 0, 0)
            outs.append(back.reshape(n_img, -1, n_tok, 2 * hd))
        return outproj(outs, weights, x, per_dev)

    def run_stage(latent, t_emb, res_norm, res_conv, res_temb, attn_norm, attn_proj):
        edge, part, t_proj = prep(latent, t_emb, res_temb)
        x, edge, part = res_block(0, latent, edge, part, t_proj, res_norm, res_conv)
        x, edge, part = attn_block(x, part, attn_norm, attn_proj)
        return res_block(1, x, edge, part, t_proj, res_norm, res_conv)[0]

    spec_x = P('dp', 'row', 'col', None)
    return jax.shard_map(run_stage, mesh=mesh, in_specs=(spec_x, P('dp', None), P(), P(), P(), P(), P()), out_specs=spec_x, check_vma=False)
```
